32 devices in a mesh: yz: 8 (over z, y), x: 4 (over x, core).
Axes of the slice: x: 2, y: 2, z: 4, core: 2. Of those that a mesh axis runs over, the one named last changes fastest.
Arguments:
- h: bfloat16 [64, 4096], P(None, ('x', 'yz'))
- g: bfloat16 [2, 4096], P(None, ('x', 'yz'))
- wq: bfloat16 [2, 4096, 4096], P(None, 'x', 'yz')
- wk: bfloat16 [2, 4096, 4096], P(None, 'x', 'yz')
- wv: bfloat16 [2, 4096, 4096], P(None, 'x', 'yz')
- w_in: bfloat16 [2, 4096, 16384], P(None, 'x', 'yz')
- wo: bfloat16 [2, 4096, 4096], P(None, 'yz', 'x')
- w_out: bfloat16 [2, 16384, 4096], P(None, 'yz', 'x')
- k_cache: bfloat16 [2, 64, 32, 256, 128], P(None, None, ('yz', 'x'))
- v_cache: bfloat16 [2, 64, 32, 256, 128], P(None, None, ('yz', 'x'))
- lens: int32 [64], replicated
Outputs:
- output 1: bfloat16 [64, 4096], P(None, ('x', 'yz'))
- output 2: bfloat16 [2, 64, 32, 128], P(None, None, ('yz', 'x'))
- output 3: bfloat16 [2, 64, 32, 128], P(None, None, ('yz', 'x'))
All inputs are finite; a program needn't handle non-finite values.
Results may differ from the reference program's by a relative error of at most 0.02.
Values are sent between devices in bfloat16 or wider.
A program may use at most 1 GiB of HBM per device.

```python
import jax
import jax.numpy as jnp
from jax import lax

E = 4096
F = 16384
H = 32
HEAD = 128
B = 64
S = 256
LAYERS = 2

EPS = 1e-6


def setup_inputs(seed: int = 0) -> dict:
    ks = jax.random.split(jax.random.PRNGKey(seed), 11)
    hd = H * HEAD
    col = 0.3 + 1.7 * jnp.arange(E, dtype=jnp.float32) / E
    h = (jax.random.normal(ks[0], (B, E), jnp.float32) * col).astype(jnp.bfloat16)
    g = (1.0 + 0.3 * jax.random.normal(ks[1], (LAYERS, E), jnp.float32)).astype(jnp.bfloat16)

    def w(k, shape, fan_in, scale=1.0):
        return (jax.random.normal(k, shape, jnp.float32) * (scale * fan_in ** -0.5)).astype(jnp.bfloat16)

    return {
        'h': h,
        'g': g,
        'wq': w(ks[2], (LAYERS, E, hd), E),
        'wk': w(ks[3], (LAYERS, E, hd), E),
        'wv': w(ks[4], (LAYERS, E, hd), E),
        'w_in': w(ks[5], (LAYERS, E, F), E),
        'wo': w(ks[6], (LAYERS, hd, E), hd, 2.0),
        'w_out': w(ks[7], (LAYERS, F, E), F),
        'k_cache': w(ks[8], (LAYERS, B, H, S, HEAD), 1, 2.0),
        'v_cache': w(ks[9], (LAYERS, B, H, S, HEAD), 1),
        'lens': jax.random.randint(ks[10], (B,), 1, S, jnp.int32),
    }


def _rope(t, pos):
    half = HEAD // 2
    inv = 10000.0 ** (-jnp.arange(half, dtype=jnp.float32) / half)
    ang = pos.astype(jnp.float32)[:, None, None] * inv
    c, s = jnp.cos(ang), jnp.sin(ang)
    tf = t.astype(jnp.float32)
    a, b = tf[..., :half], tf[..., half:]
    return jnp.concatenate([a * c - b * s, b * c + a * s], axis=-1).astype(jnp.bfloat16)


def _attend_one(args):
    q, kc, vc, k, v, ln = args
    qf = q.astype(jnp.float32)
    s = jnp.einsum('hd,hsd->hs', qf, kc.astype(jnp.float32)) * HEAD ** -0.5
    s = jnp.where(jnp.arange(S)[None, :] < ln, s, -jnp.inf)
    sn = jnp.sum(qf * k.astype(jnp.float32), axis=-1) * HEAD ** -0.5
    m = jnp.maximum(jnp.max(s, axis=-1), sn)
    p = jnp.exp(s - m[:, None])
    pn = jnp.exp(sn - m)
    den = jnp.sum(p, axis=-1) + pn
    o = jnp.einsum('hs,hsd->hd', p, vc.astype(jnp.float32)) + pn[:, None] * v.astype(jnp.float32)
    return (o / den[:, None]).astype(jnp.bfloat16)


def reference(h, g, wq, wk, wv, w_in, wo, w_out, k_cache, v_cache, lens):
    def layer(hc, xs):
        gl, wql, wkl, wvl, winl, wol, woutl, kcl, vcl = xs
        hf = hc.astype(jnp.float32)
        x = (hf * lax.rsqrt(jnp.mean(hf * hf, axis=-1, keepdims=True) + EPS) * gl.astype(jnp.float32)).astype(jnp.bfloat16)

        def proj(w):
            return jnp.dot(x, w, preferred_element_type=jnp.float32).astype(jnp.bfloat16)

        q = _rope(proj(wql).reshape(B, H, HEAD), lens)
        k = _rope(proj(wkl).reshape(B, H, HEAD), lens)
        v = proj(wvl).reshape(B, H, HEAD)
        f = jax.nn.gelu(proj(winl).astype(jnp.float32), approximate=True).astype(jnp.bfloat16)
        o = lax.map(_attend_one, (q, kcl, vcl, k, v, lens)).reshape(B, H * HEAD)
        y = (jnp.dot(o, wol, preferred_element_type=jnp.float32)
             + jnp.dot(f, woutl, preferred_element_type=jnp.float32)).astype(jnp.bfloat16)
        hn = (hf + y.astype(jnp.float32)).astype(jnp.bfloat16)
        return hn, (k, v)

    h_out, (k_new, v_new) = lax.scan(layer, h, (g, wq, wk, wv, w_in, wo, w_out, k_cache, v_cache))
    return (h_out, k_new, v_new)
```

```python
import functools
import math

import numpy as np

import jax
import jax.numpy as jnp
from jax import lax
from jax.experimental import pallas as pl
from jax.experimental.pallas import tpu as pltpu
from jax.sharding import PartitionSpec as P

EPS = 1e-6
MESH = pl.DeviceIdType.MESH
F32 = jnp.float32
BF16 = jnp.bfloat16


def _gelu(x):
    return 0.5 * x * (1.0 + jnp.tanh(math.sqrt(2.0 / math.pi) * (x + 0.044715 * (x * x * x))))


def _kernel(X, Y, e_total, h_ref, g_ref, lens_ref, inv_ref, wq, wk, wv, w_in, wo, w_out, kc, vc,
            h_out, k_out, v_out,
            wqkv_b, win_b, wo_b, wout_b, k_b, v_b,
            hcur, hbuf, gbuf, ssown, ssbuf, xs, cos_b, sin_b, lenb,
            pq, pf, rq, rf, q_b, sc_b, of32, obuf, fbuf, ybuf, ry,
            wsem, bsend, hrecv, grecv, ssend, srecv, psend, precv, asend, arecv, ysend, yrecv):
    me_y = lax.axis_index("yz")
    me_x = lax.axis_index("x")
    me = me_y * X + me_x
    N = X * Y
    L = wqkv_b.shape[0]
    B, BLK = h_ref.shape
    S, D = kc.shape[2], kc.shape[3]
    E = wq.shape[1]
    HD = wq.shape[2]
    FL = w_in.shape[2]
    FB = FL // X
    half = D // 2

    def load(l):
        out = []
        for i, w in enumerate((wq, wk, wv)):
            out.append(pltpu.make_async_copy(w.at[l], wqkv_b.at[l, :, pl.ds(i * HD, HD)], wsem.at[l, 0]))
        ce = E // 4
        for i in range(4):
            rows = pl.ds(i * ce, ce)
            out.append(pltpu.make_async_copy(w_in.at[l, rows], win_b.at[l, rows], wsem.at[l, 1]))
        cb = B // 4
        for i in range(4):
            rows = pl.ds(i * cb, cb)
            out.append(pltpu.make_async_copy(kc.at[l, rows], k_b.at[l, rows], wsem.at[l, 2]))
        for i in range(4):
            rows = pl.ds(i * cb, cb)
            out.append(pltpu.make_async_copy(vc.at[l, rows], v_b.at[l, rows], wsem.at[l, 3]))
        cf = FL // 4
        for i in range(4):
            rows = pl.ds(i * cf, cf)
            out.append(pltpu.make_async_copy(w_out.at[l, rows], wout_b.at[l, rows], wsem.at[l, 4]))
        out.append(pltpu.make_async_copy(wo.at[l], wo_b.at[l], wsem.at[l, 5]))
        return out

    def wait_bytes(ref, sem):
        pltpu.make_async_copy(ref, ref, sem).wait()

    for l in range(L):
        for c in load(l):
            c.start()

    barrier = pltpu.get_barrier_semaphore()

    def greet(d, carry):
        t = lax.rem(me + d, N)
        pl.semaphore_signal(barrier, inc=1, device_id=(lax.div(t, X), lax.rem(t, X)), device_id_type=MESH)
        return carry

    lax.fori_loop(1, N, greet, 0)

    hcur[...] = h_ref[...]
    gbuf[me_y] = g_ref[...]

    row = lax.broadcasted_iota(jnp.int32, (B, D), 0)
    lane = lax.broadcasted_iota(jnp.int32, (B, D), 1)

    def column(r):
        return jnp.sum(jnp.where(row == lane, jnp.broadcast_to(r, (B, D)), 0.0), axis=1, keepdims=True)

    lens_row = jnp.concatenate([lens_ref[...].astype(F32), jnp.zeros((1, D - B), F32)], axis=1)
    lens_col = column(lens_row)
    lenb[...] = jnp.broadcast_to(lens_col, (B, D))
    ang = lens_col * inv_ref[...]
    cos_b[...] = jnp.cos(ang)
    sn = jnp.sin(ang)
    sin_b[...] = jnp.where(lane < half, -sn, sn)

    pl.semaphore_wait(barrier, N - 1)

    def rope(t):
        tf = t.astype(F32)
        return (tf * cos_b[...] + pltpu.roll(tf, half, 1) * sin_b[...]).astype(BF16)

    def layer(l, carry):
        for d in range(1, Y):
            t = lax.rem(me_y + d, Y)
            pltpu.make_async_remote_copy(hcur, hbuf.at[l, me_y], bsend.at[l], hrecv.at[l],
                                         device_id=(t, me_x), device_id_type=MESH).start()

        @pl.when(l == 0)
        def _():
            for d in range(1, Y):
                t = lax.rem(me_y + d, Y)
                pltpu.make_async_remote_copy(g_ref, gbuf.at[me_y], bsend.at[L], grecv,
                                             device_id=(t, me_x), device_id_type=MESH).start()

        hf = hcur[...].astype(F32)
        sq = hf * hf
        col = jnp.sum(sq, axis=1, keepdims=True)
        ssown[l] = jnp.sum(jnp.where(row == lane, jnp.broadcast_to(col, (B, D)), 0.0), axis=0, keepdims=True)

        def send_ss(d, carry):
            t = lax.rem(me + d, N)
            pltpu.make_async_remote_copy(ssown.at[l], ssbuf.at[l, d - 1], ssend.at[l], srecv.at[l],
                                         device_id=(lax.div(t, X), lax.rem(t, X)), device_id_type=MESH).start()
            return carry

        lax.fori_loop(1, N, send_ss, 0)
        hbuf[l, me_y] = hcur[...]

        wait_bytes(hbuf.at[l, pl.ds(0, Y - 1)], hrecv.at[l])

        @pl.when(l == 0)
        def _():
            wait_bytes(gbuf.at[pl.ds(0, Y - 1)], grecv)

        wait_bytes(ssbuf.at[l], srecv.at[l])
        tot = jnp.sum(ssbuf[l], axis=0) + ssown[l]
        r = lax.rsqrt(column(tot) / e_total + EPS)
        for j in range(Y):
            gl = gbuf[j, pl.ds(l, 1), :].astype(F32)
            xs[:, j * BLK:(j + 1) * BLK] = (hbuf[l, j].astype(F32) * r * gl).astype(BF16)

        wait_bytes(wqkv_b.at[l], wsem.at[l, 0])
        for i in range(3):
            p = jnp.dot(xs[...], wqkv_b[l, :, i * HD:(i + 1) * HD], preferred_element_type=F32).astype(BF16)
            for j in range(X):
                pq[l, j, :, i * D:(i + 1) * D] = p[:, j * D:(j + 1) * D]
        for d in range(1, X):
            t = lax.rem(me_x + d, X)
            pltpu.make_async_remote_copy(pq.at[l, t], rq.at[l, d - 1], psend.at[l, 0], precv.at[l, 0],
                                         device_id=(me_y, t), device_id_type=MESH).start()
        wait_bytes(win_b.at[l], wsem.at[l, 1])
        for j in range(X):
            pf[l, j] = jnp.dot(xs[...], win_b[l, :, j * FB:(j + 1) * FB], preferred_element_type=F32).astype(BF16)
        for d in range(1, X):
            t = lax.rem(me_x + d, X)
            pltpu.make_async_remote_copy(pf.at[l, t], rf.at[l, d - 1], psend.at[l, 1], precv.at[l, 1],
                                         device_id=(me_y, t), device_id_type=MESH).start()

        wait_bytes(rq.at[l], precv.at[l, 0])
        s = pq[l, me_x].astype(F32)
        for d in range(X - 1):
            s = s + rq[l, d].astype(F32)
        q = rope(s[:, :D].astype(BF16))
        k = rope(s[:, D:2 * D].astype(BF16))
        v = s[:, 2 * D:].astype(BF16)
        q_b[...] = q
        k_out[l] = k
        v_out[l] = v

        wait_bytes(rf.at[l], precv.at[l, 1])
        s = pf[l, me_x].astype(F32)
        for d in range(X - 1):
            s = s + rf[l, d].astype(F32)
        fbuf[l, me_x] = _gelu(s.astype(BF16).astype(F32)).astype(BF16)
        for d in range(1, X):
            t = lax.rem(me_x + d, X)
            pltpu.make_async_remote_copy(fbuf.at[l, me_x], fbuf.at[l, me_x], asend.at[l, 0], arecv.at[l, 0],
                                         device_id=(me_y, t), device_id_type=MESH).start()

        scale = D ** -0.5
        wait_bytes(k_b.at[l], wsem.at[l, 2])
        G = 16
        grow = lax.broadcasted_iota(jnp.int32, (G, S), 0)

        def scores(i, carry):
            b0 = pl.multiple_of(i * G, G)
            qg = q_b[pl.ds(b0, G), :]
            acc = jnp.zeros((G, S), F32)
            for j in range(G):
                t = lax.dot_general(qg, k_b[l, b0 + j], (((1,), (1,)), ((), ())), preferred_element_type=F32)
                acc = jnp.where(grow == j, t, acc)
            sc_b[pl.ds(b0, G), :] = acc
            return carry

        lax.fori_loop(0, B // G, scores, 0)
        sc = sc_b[...] * scale
        pos = lax.broadcasted_iota(jnp.int32, (B, S), 1).astype(F32)
        lc = lenb[...]
        sc = jnp.where(pos < jnp.concatenate([lc] * (S // D), axis=1), sc, -jnp.inf)
        sn = jnp.sum(q.astype(F32) * k.astype(F32), axis=1, keepdims=True) * scale
        m = jnp.maximum(jnp.max(sc, axis=1, keepdims=True), sn)
        p = jnp.exp(sc - m)
        pn = jnp.exp(sn - m)
        den = jnp.sum(p, axis=1, keepdims=True) + pn
        sc_b[...] = p
        wait_bytes(v_b.at[l], wsem.at[l, 3])
        orow = lax.broadcasted_iota(jnp.int32, (G, D), 0)

        def values(i, carry):
            b0 = pl.multiple_of(i * G, G)
            pg = sc_b[pl.ds(b0, G), :].astype(BF16)
            acc = jnp.zeros((G, D), F32)
            for j in range(G):
                t = jnp.dot(pg, v_b[l, b0 + j], preferred_element_type=F32)
                acc = jnp.where(orow == j, t, acc)
            of32[pl.ds(b0, G), :] = acc
            return carry

        lax.fori_loop(0, B // G, values, 0)
        o = of32[...] + pn * v.astype(F32)
        obuf[l, me_x] = (o / den).astype(BF16)
        for d in range(1, X):
            t = lax.rem(me_x + d, X)
            pltpu.make_async_remote_copy(obuf.at[l, me_x], obuf.at[l, me_x], asend.at[l, 1], arecv.at[l, 1],
                                         device_id=(me_y, t), device_id_type=MESH).start()

        wait_bytes(wout_b.at[l], wsem.at[l, 4])
        wait_bytes(fbuf.at[l, pl.ds(0, X - 1)], arecv.at[l, 0])
        wait_bytes(wo_b.at[l], wsem.at[l, 5])
        wait_bytes(obuf.at[l, pl.ds(0, X - 1)], arecv.at[l, 1])
        W = 2 * BLK
        for n in range(Y * BLK // W):
            cols = slice(n * W, (n + 1) * W)
            acc = jnp.zeros((B, W), F32)
            for j in range(X):
                acc = acc + jnp.dot(fbuf[l, j], wout_b[l, j * FB:(j + 1) * FB, cols], preferred_element_type=F32)
                acc = acc + jnp.dot(obuf[l, j], wo_b[l, j * D:(j + 1) * D, cols], preferred_element_type=F32)
            ybuf[l, 2 * n] = acc[:, :BLK].astype(BF16)
            ybuf[l, 2 * n + 1] = acc[:, BLK:].astype(BF16)
        for d in range(1, Y):
            t = lax.rem(me_y + d, Y)
            pltpu.make_async_remote_copy(ybuf.at[l, t], ry.at[l, d - 1], ysend.at[l], yrecv.at[l],
                                         device_id=(t, me_x), device_id_type=MESH).start()
        wait_bytes(ry.at[l], yrecv.at[l])
        y = ybuf[l, me_y].astype(F32)
        for d in range(Y - 1):
            y = y + ry[l, d].astype(F32)
        wait_bytes(hbuf.at[l, pl.ds(0, Y - 1)], bsend.at[l])
        hcur[...] = (hcur[...].astype(F32) + y.astype(BF16).astype(F32)).astype(BF16)
        return carry

    for l in range(L):
        layer(l, 0)
    h_out[...] = hcur[...]

    for l in range(L):
        wait_bytes(ssbuf.at[l], ssend.at[l])
        wait_bytes(rq.at[l], psend.at[l, 0])
        wait_bytes(rf.at[l], psend.at[l, 1])
        wait_bytes(fbuf.at[l, pl.ds(0, X - 1)], asend.at[l, 0])
        wait_bytes(obuf.at[l, pl.ds(0, X - 1)], asend.at[l, 1])
        wait_bytes(ry.at[l], ysend.at[l])
    wait_bytes(gbuf.at[pl.ds(0, Y - 1)], bsend.at[L])


def solution(mesh):
    X = mesh.shape['x']
    Y = mesh.shape['yz']
    act = P(None, ('x', 'yz'))
    w_first = P(None, 'x', 'yz')
    w_second = P(None, 'yz', 'x')
    cache = P(None, None, ('yz', 'x'), None, None)
    new = P(None, None, ('yz', 'x'), None)

    def body(h, g, wq, wk, wv, w_in, wo, w_out, kc, vc, lens):
        B, BLK = h.shape
        L, E, HD = wq.shape
        FL = w_in.shape[2]
        FB = FL // X
        S, D = kc.shape[3], kc.shape[4]
        half = D // 2
        kc = kc.reshape(L, B, S, D)
        vc = vc.reshape(L, B, S, D)
        i = np.arange(half, dtype=np.float32)
        inv = np.power(np.float32(10000.0), -i / np.float32(half)).astype(np.float32)
        inv = jnp.asarray(np.concatenate([inv, inv])[None])
        vm = pl.BlockSpec(memory_space=pltpu.VMEM)
        hbm = pl.BlockSpec(memory_space=pl.ANY)
        N = X * Y
        dma = pltpu.SemaphoreType.DMA
        scratch = [
            pltpu.VMEM((L, E, 3 * HD), BF16), pltpu.VMEM((L, E, FL), BF16),
            pltpu.VMEM((L, HD, E), BF16), pltpu.VMEM((L, FL, E), BF16),
            pltpu.VMEM((L, B, S, D), BF16), pltpu.VMEM((L, B, S, D), BF16),
            pltpu.VMEM((B, BLK), BF16), pltpu.VMEM((L, Y, B, BLK), BF16), pltpu.VMEM((Y, L, BLK), BF16),
            pltpu.VMEM((L, 1, D), F32), pltpu.VMEM((L, N - 1, 1, D), F32), pltpu.VMEM((B, Y * BLK), BF16),
            pltpu.VMEM((B, D), F32), pltpu.VMEM((B, D), F32), pltpu.VMEM((B, D), F32),
            pltpu.VMEM((L, X, B, 3 * D), BF16), pltpu.VMEM((L, X, B, FB), BF16),
            pltpu.VMEM((L, X - 1, B, 3 * D), BF16), pltpu.VMEM((L, X - 1, B, FB), BF16),
            pltpu.VMEM((B, D), BF16), pltpu.VMEM((B, S), F32), pltpu.VMEM((B, D), F32),
            pltpu.VMEM((L, X, B, D), BF16), pltpu.VMEM((L, X, B, FB), BF16),
            pltpu.VMEM((L, Y, B, BLK), BF16), pltpu.VMEM((L, Y - 1, B, BLK), BF16),
            dma((L, 6)), dma((L + 1,)), dma((L,)), dma, dma((L,)), dma((L,)),
            dma((L, 2)), dma((L, 2)), dma((L, 2)), dma((L, 2)), dma((L,)), dma((L,)),
        ]
        h_new, k_new, v_new = pl.pallas_call(
            functools.partial(_kernel, X, Y, float(BLK * N)),
            out_shape=(jax.ShapeDtypeStruct((B, BLK), BF16),
                       jax.ShapeDtypeStruct((L, B, D), BF16),
                       jax.ShapeDtypeStruct((L, B, D), BF16)),
            in_specs=[vm] * 4 + [hbm] * 8,
            out_specs=(vm, vm, vm),
            scratch_shapes=scratch,
            compiler_params=pltpu.CompilerParams(
                collective_id=0, has_side_effects=True, vmem_limit_bytes=67043328),
            name="decode_step",
        )(h, g, lens.reshape(1, B), inv, wq, wk, wv, w_in, wo, w_out, kc, vc)
        return h_new, k_new.reshape(L, B, 1, D), v_new.reshape(L, B, 1, D)

    return jax.shard_map(
        body, mesh=mesh,
        in_specs=(act, act, w_first, w_first, w_first, w_first, w_second, w_second, cache, cache, P(None)),
        out_specs=(act, new, new), check_vma=False)
```

```python
import functools
import math

import numpy as np

import jax
import jax.numpy as jnp
from jax import lax
from jax.experimental import pallas as pl
from jax.experimental.pallas import tpu as pltpu
from jax.sharding import PartitionSpec as P

EPS = 1e-6
MESH = pl.DeviceIdType.MESH
F32 = jnp.float32
BF16 = jnp.bfloat16
CH = 2


def _gelu(x):
    return 0.5 * x * (1.0 + jnp.tanh(math.sqrt(2.0 / math.pi) * (x + 0.044715 * (x * x * x))))


def _partner(i, mask):
    bit = 1
    t = i
    while bit <= mask:
        if mask & bit:
            t = t + bit * (1 - 2 * lax.rem(lax.div(i, bit), 2))
        bit *= 2
    return t


def _kernel(X, Y, e_total, h_ref, g_ref, lens_ref, inv_ref, wq, wk, wv, w_in, wo, w_out, kc, vc,
            h_out, k_out, v_out,
            wqkv_b, win_b, wo_b, wout_b, k_b, v_b,
            hcur, hbuf, gown, gbuf, lens_b, inv_b, ssown, ssbuf, xs, cos_b, sin_b, lenb,
            pq, pkv, rq, rkv, q_b, sc_b, of32, obuf,
            fsib, fsibr, fown, fcross, fcrossr, fbuf, yacc, ybuf, ry,
            isem, wsem, hsend, hrecv, gsend, grecv, ssend, srecv, qsend, qrecv,
            asend, arecv, bsend, brecv, csend, crecv, osend, orecv, ysend, yrecv):
    me_y = lax.axis_index("yz")
    me_x = lax.axis_index("x")
    me = me_y * X + me_x
    N = X * Y
    L = wqkv_b.shape[0]
    B, BLK = h_ref.shape
    S, D = kc.shape[2], kc.shape[3]
    E = wq.shape[1]
    HD = wq.shape[2]
    FL = w_in.shape[2]
    FH = FL // 2
    CW = FH // CH
    half = D // 2
    core = lax.rem(me_x, 2)
    sib = _partner(me_x, 1)
    cross = _partner(me_x, 2)
    masks = list(range(Y - 1, 0, -1))

    def remote(src, dst, send, recv, y, x):
        pltpu.make_async_remote_copy(src, dst, send, recv, device_id=(y, x), device_id_type=MESH).start()

    def wait_bytes(ref, sem, name="wait"):
        with jax.named_scope(name):
            pltpu.make_async_copy(ref, ref, sem).wait()

    inputs = [pltpu.make_async_copy(s, d, isem.at[i]) for i, (s, d) in enumerate(
        ((h_ref, hcur), (g_ref, gown), (lens_ref, lens_b), (inv_ref, inv_b)))]
    for c in inputs:
        c.start()

    barrier = pltpu.get_barrier_semaphore()

    def greet(d, carry):
        t = lax.rem(me + d, N)
        pl.semaphore_signal(barrier, inc=1, device_id=(lax.div(t, X), lax.rem(t, X)), device_id_type=MESH)
        return carry

    lax.fori_loop(1, N, greet, 0)

    def load(l):
        for i, w in enumerate((wq, wk, wv)):
            pltpu.make_async_copy(w.at[l], wqkv_b.at[l, :, pl.ds(i * HD, HD)], wsem.at[l, 0]).start()
        for i, (w, b) in enumerate(((w_in, win_b), (kc, k_b), (vc, v_b), (w_out, wout_b))):
            n = w.shape[1] // 4
            for j in range(4):
                rows = pl.ds(j * n, n)
                pltpu.make_async_copy(w.at[l, rows], b.at[l, rows], wsem.at[l, i + 1]).start()
        pltpu.make_async_copy(wo.at[l], wo_b.at[l], wsem.at[l, 5]).start()

    for c in inputs:
        c.wait()
    for l in range(L):
        load(l)
    gbuf[me_y] = gown[...]

    row = lax.broadcasted_iota(jnp.int32, (B, D), 0)
    lane = lax.broadcasted_iota(jnp.int32, (B, D), 1)

    def column(r):
        return jnp.sum(jnp.where(row == lane, jnp.broadcast_to(r, (B, D)), 0.0), axis=1, keepdims=True)

    def as_row(c):
        return jnp.sum(jnp.where(row == lane, jnp.broadcast_to(c, (B, D)), 0.0), axis=0, keepdims=True)

    lens_row = jnp.concatenate([lens_b[...].astype(F32), jnp.zeros((1, D - B), F32)], axis=1)
    lens_col = column(lens_row)
    lenb[...] = jnp.broadcast_to(lens_col, (B, D))
    ang = lens_col * inv_b[...]
    cos_b[...] = jnp.cos(ang)
    sn = jnp.sin(ang)
    sin_b[...] = jnp.where(lane < half, -sn, sn)

    def rope(t):
        tf = t.astype(F32)
        return (tf * cos_b[...] + pltpu.roll(tf, half, 1) * sin_b[...]).astype(BF16)

    def send_h(l):
        for m in masks:
            remote(hcur, hbuf.at[l, me_y], hsend.at[l], hrecv.at[l], _partner(me_y, m), me_x)
        hf = hcur[...].astype(F32)
        ssown[l] = as_row(jnp.sum(hf * hf, axis=1, keepdims=True))

        def send_ss(d, carry):
            t = lax.rem(me + d, N)
            remote(ssown.at[l], ssbuf.at[l, d - 1], ssend.at[l], srecv.at[l], lax.div(t, X), lax.rem(t, X))
            return carry

        lax.fori_loop(1, N, send_ss, 0)
        hbuf[l, me_y] = hcur[...]

    with jax.named_scope("w_bar"):
        pl.semaphore_wait(barrier, N - 1)
    for m in masks:
        remote(gown, gbuf.at[me_y], gsend, grecv, _partner(me_y, m), me_x)

    for l in range(L):
        send_h(l)
        if l == 0:
            wait_bytes(gbuf.at[pl.ds(0, Y - 1)], grecv)
        wait_bytes(hbuf.at[l, pl.ds(0, Y - 1)], hrecv.at[l], "w_h")
        wait_bytes(ssbuf.at[l], srecv.at[l], "w_ss")
        tot = jnp.sum(ssbuf[l], axis=0) + ssown[l]
        r = lax.rsqrt(column(tot) / e_total + EPS)
        for j in range(Y):
            gl = gbuf[j, pl.ds(l, 1), :].astype(F32)
            xs[:, j * BLK:(j + 1) * BLK] = (hbuf[l, j].astype(F32) * r * gl).astype(BF16)

        wait_bytes(wqkv_b.at[l], wsem.at[l, 0], "w_wqkv")

        def part(i):
            return jnp.dot(xs[...], wqkv_b[l, :, i * HD:(i + 1) * HD], preferred_element_type=F32).astype(BF16)

        p = part(0)
        for j in range(X):
            pq[l, j] = p[:, j * D:(j + 1) * D]
        for m in (2, 3, 1):
            t = _partner(me_x, m)
            remote(pq.at[l, t], rq.at[l, m - 1], qsend.at[l, 0], qrecv.at[l, 0], me_y, t)
        for i in range(2):
            p = part(i + 1)
            for j in range(X):
                pkv[l, j, :, i * D:(i + 1) * D] = p[:, j * D:(j + 1) * D]
        for m in (2, 3, 1):
            t = _partner(me_x, m)
            remote(pkv.at[l, t], rkv.at[l, m - 1], qsend.at[l, 1], qrecv.at[l, 1], me_y, t)

        wait_bytes(win_b.at[l], wsem.at[l, 1], "w_win")
        for i in range(CH):
            cols = pl.ds(pl.multiple_of((1 - core) * FH + i * CW, CW), CW)
            fsib[l, i] = jnp.dot(xs[...], win_b[l, :, cols], preferred_element_type=F32).astype(BF16)
            remote(fsib.at[l, i], fsibr.at[l, i], asend.at[l, i], arecv.at[l, i], me_y, sib)
        for i in range(CH):
            cols = pl.ds(pl.multiple_of(core * FH + i * CW, CW), CW)
            fown[i] = jnp.dot(xs[...], win_b[l, :, cols], preferred_element_type=F32)
        for i in range(CH):
            wait_bytes(fsibr.at[l, i], arecv.at[l, i], "w_fs")
            s = fown[i] + fsibr[l, i].astype(F32)
            fown[i] = s
            fcross[l, i] = s.astype(BF16)
            remote(fcross.at[l, i], fcrossr.at[l, i], bsend.at[l, i], brecv.at[l, i], me_y, cross)

        scale = D ** -0.5
        wait_bytes(k_b.at[l], wsem.at[l, 2], "w_k")
        wait_bytes(rq.at[l], qrecv.at[l, 0], "w_q")
        s = pq[l, me_x].astype(F32)
        for d in range(X - 1):
            s = s + rq[l, d].astype(F32)
        q = rope(s.astype(BF16))
        q_b[...] = q
        G = 16
        grow = lax.broadcasted_iota(jnp.int32, (G, S), 0)
        for i in range(B // G):
            b0 = i * G
            qg = q_b[b0:b0 + G, :]
            acc = jnp.zeros((G, S), F32)
            for j in range(G):
                t = lax.dot_general(qg, k_b[l, b0 + j], (((1,), (1,)), ((), ())), preferred_element_type=F32)
                acc = jnp.where(grow == j, t, acc)
            sc_b[b0:b0 + G, :] = acc
        wait_bytes(rkv.at[l], qrecv.at[l, 1], "w_kv")
        s = pkv[l, me_x].astype(F32)
        for d in range(X - 1):
            s = s + rkv[l, d].astype(F32)
        k = rope(s[:, :D].astype(BF16))
        v = s[:, D:].astype(BF16)
        k_out[l] = k
        v_out[l] = v
        sc = sc_b[...] * scale
        pos = lax.broadcasted_iota(jnp.int32, (B, S), 1).astype(F32)
        sc = jnp.where(pos < jnp.concatenate([lenb[...]] * (S // D), axis=1), sc, -jnp.inf)
        sn = jnp.sum(q.astype(F32) * k.astype(F32), axis=1, keepdims=True) * scale
        m = jnp.maximum(jnp.max(sc, axis=1, keepdims=True), sn)
        p = jnp.exp(sc - m)
        pn = jnp.exp(sn - m)
        den = jnp.sum(p, axis=1, keepdims=True) + pn
        sc_b[...] = p
        wait_bytes(v_b.at[l], wsem.at[l, 3], "w_v")
        orow = lax.broadcasted_iota(jnp.int32, (G, D), 0)
        for i in range(B // G):
            b0 = i * G
            pg = sc_b[b0:b0 + G, :].astype(BF16)
            acc = jnp.zeros((G, D), F32)
            for j in range(G):
                t = jnp.dot(pg, v_b[l, b0 + j], preferred_element_type=F32)
                acc = jnp.where(orow == j, t, acc)
            of32[b0:b0 + G, :] = acc
        o = of32[...] + pn * v.astype(F32)
        obuf[l, me_x] = (o / den).astype(BF16)
        for m in (2, 3, 1):
            t = _partner(me_x, m)
            remote(obuf.at[l, me_x], obuf.at[l, me_x], osend.at[l], orecv.at[l], me_y, t)

        for i in range(CH):
            wait_bytes(fcrossr.at[l, i], brecv.at[l, i], "w_fc")
            s = fown[i] + fcrossr[l, i].astype(F32)
            c = core * CH + i
            fbuf[l, c] = _gelu(s.astype(BF16).astype(F32)).astype(BF16)
            remote(fbuf.at[l, c], fbuf.at[l, c], csend.at[l, i], crecv.at[l, i], me_y, sib)

        wait_bytes(wout_b.at[l], wsem.at[l, 4], "w_wout")

        def f_dot(c0):
            f = jnp.concatenate([fbuf[l, c0 + i] for i in range(CH)], axis=1)
            rows = pl.ds(pl.multiple_of(c0 * CW, CW), FH)
            return jnp.dot(f, wout_b[l, rows, :], preferred_element_type=F32)

        yacc[...] = f_dot(core * CH)
        for i in range(CH):
            wait_bytes(fbuf.at[l, i], crecv.at[l, i], "w_fg")
        yacc[...] = yacc[...] + f_dot((1 - core) * CH)
        wait_bytes(wo_b.at[l], wsem.at[l, 5], "w_wo")
        wait_bytes(obuf.at[l, pl.ds(0, X - 1)], orecv.at[l], "w_og")
        og = jnp.concatenate([obuf[l, j] for j in range(X)], axis=1)
        for m in masks[::2]:
            z = lax.div(_partner(me_y, m), 2)
            cols = pl.ds(pl.multiple_of(z * 2 * BLK, 2 * BLK), 2 * BLK)
            acc = yacc[:, cols] + jnp.dot(og, wo_b[l, :, cols], preferred_element_type=F32)
            ybuf[l, 2 * z] = acc[:, :BLK].astype(BF16)
            ybuf[l, 2 * z + 1] = acc[:, BLK:].astype(BF16)
            for n in (m, m - 1) if m > 1 else (m,):
                t = _partner(me_y, n)
                remote(ybuf.at[l, t], ry.at[l, n - 1], ysend.at[l], yrecv.at[l], t, me_x)
        wait_bytes(hbuf.at[l, pl.ds(0, Y - 1)], hsend.at[l])
        wait_bytes(ry.at[l], yrecv.at[l], "w_y")
        y = ybuf[l, me_y].astype(F32)
        for d in range(Y - 1):
            y = y + ry[l, d].astype(F32)
        hcur[...] = (hcur[...].astype(F32) + y.astype(BF16).astype(F32)).astype(BF16)
    h_out[...] = hcur[...]

    for l in range(L):
        wait_bytes(ssbuf.at[l], ssend.at[l])
        wait_bytes(rq.at[l], qsend.at[l, 0])
        wait_bytes(rkv.at[l], qsend.at[l, 1])
        for i in range(CH):
            wait_bytes(fsib.at[l, i], asend.at[l, i])
            wait_bytes(fcross.at[l, i], bsend.at[l, i])
            wait_bytes(fbuf.at[l, i], csend.at[l, i])
        wait_bytes(obuf.at[l, pl.ds(0, X - 1)], osend.at[l])
        wait_bytes(ry.at[l], ysend.at[l])
    wait_bytes(gbuf.at[pl.ds(0, Y - 1)], gsend)


def _finish(h, k, v, h_out, k_out, v_out, sem):
    copies = [pltpu.make_async_copy(a, b, sem.at[i]) for i, (a, b) in enumerate(((k, k_out), (v, v_out), (h, h_out)))]
    for c in copies:
        c.start()
    for c in copies:
        c.wait()


def solution(mesh):
    X = mesh.shape['x']
    Y = mesh.shape['yz']
    act = P(None, ('x', 'yz'))
    w_first = P(None, 'x', 'yz')
    w_second = P(None, 'yz', 'x')
    cache = P(None, None, ('yz', 'x'), None, None)
    new = P(None, None, ('yz', 'x'), None)

    def body(h, g, wq, wk, wv, w_in, wo, w_out, kc, vc, lens):
        B, BLK = h.shape
        L, E, HD = wq.shape
        FL = w_in.shape[2]
        S, D = kc.shape[3], kc.shape[4]
        half = D // 2
        CW = FL // 2 // CH
        kc = kc.reshape(L, B, S, D)
        vc = vc.reshape(L, B, S, D)
        i = np.arange(half, dtype=np.float32)
        inv = np.power(np.float32(10000.0), -i / np.float32(half)).astype(np.float32)
        inv = jnp.asarray(np.concatenate([inv, inv])[None])
        vm = pl.BlockSpec(memory_space=pltpu.VMEM)
        hbm = pl.BlockSpec(memory_space=pl.ANY)
        far = pl.BlockSpec(memory_space=pltpu.HBM)
        N = X * Y
        dma = pltpu.SemaphoreType.DMA
        V = pltpu.VMEM
        scratch = [
            V((L, E, 3 * HD), BF16), V((L, E, FL), BF16), V((L, HD, E), BF16), V((L, FL, E), BF16),
            V((L, B, S, D), BF16), V((L, B, S, D), BF16),
            V((B, BLK), BF16), V((L, Y, B, BLK), BF16), V((L, BLK), BF16), V((Y, L, BLK), BF16),
            V((1, B), jnp.int32), V((1, D), F32),
            V((L, 1, D), F32), V((L, N - 1, 1, D), F32), V((B, Y * BLK), BF16),
            V((B, D), F32), V((B, D), F32), V((B, D), F32),
            V((L, X, B, D), BF16), V((L, X, B, 2 * D), BF16),
            V((L, X - 1, B, D), BF16), V((L, X - 1, B, 2 * D), BF16),
            V((B, D), BF16), V((B, S), F32), V((B, D), F32), V((L, X, B, D), BF16),
            V((L, CH, B, CW), BF16), V((L, CH, B, CW), BF16), V((CH, B, CW), F32),
            V((L, CH, B, CW), BF16), V((L, CH, B, CW), BF16), V((L, 2 * CH, B, CW), BF16),
            V((B, Y * BLK), F32), V((L, Y, B, BLK), BF16), V((L, Y - 1, B, BLK), BF16),
            dma((4,)), dma((L, 6)), dma((L,)), dma((L,)), dma, dma, dma((L,)), dma((L,)), dma((L, 2)), dma((L, 2)),
            dma((L, CH)), dma((L, CH)), dma((L, CH)), dma((L, CH)), dma((L, CH)), dma((L, CH)),
            dma((L,)), dma((L,)), dma((L,)), dma((L,)),
        ]
        shapes = (jax.ShapeDtypeStruct((B, BLK), BF16),
                  jax.ShapeDtypeStruct((L, B, D), BF16),
                  jax.ShapeDtypeStruct((L, B, D), BF16))
        outs = pl.pallas_call(
            functools.partial(_kernel, X, Y, float(BLK * N)),
            out_shape=tuple(V(t.shape, t.dtype) for t in shapes),
            in_specs=[hbm] * 12,
            out_specs=(vm, vm, vm),
            scratch_shapes=scratch,
            compiler_params=pltpu.CompilerParams(
                collective_id=0, has_side_effects=True, vmem_limit_bytes=56 * 1024 * 1024),
            name="decode_step",
        )(h, g, lens.reshape(1, B), inv, wq, wk, wv, w_in, wo, w_out, kc, vc)
        h_new, k_new, v_new = pl.pallas_call(
            _finish, out_shape=shapes, in_specs=[vm] * 3, out_specs=(far, far, far), name="finish",
            scratch_shapes=[dma((3,))],
        )(*[pltpu.with_memory_space_constraint(t, pltpu.VMEM) for t in outs])
        return h_new, k_new.reshape(L, B, 1, D), v_new.reshape(L, B, 1, D)

    return jax.shard_map(
        body, mesh=mesh,
        in_specs=(act, act, w_first, w_first, w_first, w_first, w_second, w_second, cache, cache, P(None)),
        out_specs=(act, new, new), check_vma=False)
```

```python
import functools
import math

import numpy as np

import jax
import jax.numpy as jnp
from jax import lax
from jax.experimental import pallas as pl
from jax.experimental.pallas import tpu as pltpu
from jax.sharding import PartitionSpec as P

EPS = 1e-6
MESH = pl.DeviceIdType.MESH
F32 = jnp.float32
BF16 = jnp.bfloat16
CH = 2


def _gelu(x):
    return 0.5 * x * (1.0 + jnp.tanh(math.sqrt(2.0 / math.pi) * (x + 0.044715 * (x * x * x))))


def _partner(i, mask):
    bit = 1
    t = i
    while bit <= mask:
        if mask & bit:
            t = t + bit * (1 - 2 * lax.rem(lax.div(i, bit), 2))
        bit *= 2
    return t


def _kernel(X, Y, e_total, h_ref, g_ref, lens_ref, inv_ref, wq, wk, wv, w_in, wo, w_out, kc, vc,
            h_out, k_out, v_out,
            wqkv_b, win_b, wo_b, wout_b, k_b, v_b, kt_b,
            hcur, hbuf, gown, gbuf, lens_b, inv_b, ssown, ssbuf, xs, cos_b, sin_b, lenb,
            pq, pkv, rq, rkv, q_b, m_b, d_b, of32, obuf,
            fsib, fsibr, fown, fcross, fcrossr, fbuf, yacc, ybuf, ry,
            isem, wsem, hsend, hrecv, gsend, grecv, ssend, srecv, qsend, qrecv,
            asend, arecv, bsend, brecv, csend, crecv, osend, orecv, ysend, yrecv):
    me_y = lax.axis_index("yz")
    me_x = lax.axis_index("x")
    me = me_y * X + me_x
    N = X * Y
    L = wqkv_b.shape[0]
    B, BLK = h_ref.shape
    S, D = kc.shape[2], kc.shape[3]
    E = wq.shape[1]
    HD = wq.shape[2]
    FL = w_in.shape[2]
    FH = FL // 2
    CW = FH // CH
    half = D // 2
    core = lax.rem(me_x, 2)
    py = [_partner(me_y, m) for m in range(Y)]
    px = [_partner(me_x, m) for m in range(X)]
    sib, cross = px[1], px[2]
    masks = list(range(Y - 1, 0, -1))
    others = [(m, n) for m in range(Y - 1, -1, -1) for n in range(X - 1, 0, -1)]

    def remote(src, dst, send, recv, y, x):
        pltpu.make_async_remote_copy(src, dst, send, recv, device_id=(y, x), device_id_type=MESH).start()

    def wait_bytes(ref, sem, name="wait"):
        with jax.named_scope(name):
            pltpu.make_async_copy(ref, ref, sem).wait()

    inputs = [pltpu.make_async_copy(s, d, isem.at[i]) for i, (s, d) in enumerate(
        ((h_ref, hcur), (g_ref, gown), (lens_ref, lens_b), (inv_ref, inv_b)))]
    for c in inputs:
        c.start()

    barrier = pltpu.get_barrier_semaphore()

    def greet(d, carry):
        t = lax.rem(me + d, N)
        pl.semaphore_signal(barrier, inc=1, device_id=(lax.div(t, X), lax.rem(t, X)), device_id_type=MESH)
        return carry

    lax.fori_loop(1, N, greet, 0)

    def load(l):
        def rows(w, b, i, parts=4):
            n = w.shape[1] // parts
            for j in range(parts):
                pltpu.make_async_copy(w.at[l, pl.ds(j * n, n)], b.at[l, pl.ds(j * n, n)], wsem.at[l, i]).start()

        rows(kc, k_b, 2)
        for i, w in enumerate((wq, wk, wv)):
            pltpu.make_async_copy(w.at[l], wqkv_b.at[l, :, pl.ds(i * HD, HD)], wsem.at[l, 0]).start()
        rows(w_in, win_b, 1)
        rows(vc, v_b, 3)
        rows(w_out, wout_b, 4)
        rows(wo, wo_b, 5, 1)

    def transpose_k(l):
        wait_bytes(k_b.at[l], wsem.at[l, 2], "w_k")

        def step(i, carry):
            for j in range(8):
                kt_b[i * 8 + j] = k_b[l, i * 8 + j].T
            return carry

        with jax.named_scope("kt"):
            lax.fori_loop(0, B // 8, step, 0)

    for c in inputs:
        c.wait()
    for l in range(L):
        load(l)
    gbuf[me_y] = gown[...]

    row = lax.broadcasted_iota(jnp.int32, (B, D), 0)
    lane = lax.broadcasted_iota(jnp.int32, (B, D), 1)

    def column(r):
        return jnp.sum(jnp.where(row == lane, jnp.broadcast_to(r, (B, D)), 0.0), axis=1, keepdims=True)

    def as_row(c):
        return jnp.sum(jnp.where(row == lane, jnp.broadcast_to(c, (B, D)), 0.0), axis=0, keepdims=True)

    lens_row = jnp.concatenate([lens_b[...].astype(F32), jnp.zeros((1, D - B), F32)], axis=1)
    lens_col = column(lens_row)
    lenb[...] = jnp.broadcast_to(lens_col, (B, D))
    ang = lens_col * inv_b[...]
    cos_b[...] = jnp.cos(ang)
    sn = jnp.sin(ang)
    sin_b[...] = jnp.where(lane < half, -sn, sn)

    def rope(t):
        tf = t.astype(F32)
        return (tf * cos_b[...] + pltpu.roll(tf, half, 1) * sin_b[...]).astype(BF16)

    def send_h(l):
        hf = hcur[...].astype(F32)
        ssown[l] = as_row(jnp.sum(hf * hf, axis=1, keepdims=True))
        for i, (m, n) in enumerate(others):
            remote(ssown.at[l], ssbuf.at[l, i], ssend.at[l], srecv.at[l], py[m], px[n])
        for m in masks:
            remote(hcur, hbuf.at[l, me_y], hsend.at[l], hrecv.at[l], py[m], me_x)
        hbuf[l, me_y] = hcur[...]

    with jax.named_scope("w_bar"):
        pl.semaphore_wait(barrier, N - 1)
    for m in masks:
        remote(gown, gbuf.at[me_y], gsend, grecv, py[m], me_x)

    for l in range(L):
        send_h(l)
        if l == 0:
            transpose_k(0)
            wait_bytes(gbuf.at[pl.ds(0, Y - 1)], grecv)
        wait_bytes(hbuf.at[l, pl.ds(0, Y - 1)], hrecv.at[l], "w_h")
        wait_bytes(ssbuf.at[l], srecv.at[l], "w_ss")
        row_ss = jnp.zeros((B, BLK), F32)
        for j in range(Y):
            hf = hbuf[l, j].astype(F32)
            row_ss = row_ss + hf * hf
        tot = jnp.sum(row_ss, axis=1, keepdims=True) + column(jnp.sum(ssbuf[l], axis=0))
        r = lax.rsqrt(tot / e_total + EPS)
        for j in range(Y):
            gl = gbuf[j, pl.ds(l, 1), :].astype(F32)
            xs[:, j * BLK:(j + 1) * BLK] = (hbuf[l, j].astype(F32) * r * gl).astype(BF16)

        wait_bytes(wqkv_b.at[l], wsem.at[l, 0], "w_wqkv")

        def part(i):
            return jnp.dot(xs[...], wqkv_b[l, :, i * HD:(i + 1) * HD], preferred_element_type=F32).astype(BF16)

        p = part(0)
        for j in range(X):
            pq[l, j] = p[:, j * D:(j + 1) * D]
        for m in (2, 3, 1):
            t = px[m]
            remote(pq.at[l, t], rq.at[l, m - 1], qsend.at[l, 0], qrecv.at[l, 0], me_y, t)
        for i in range(2):
            p = part(i + 1)
            for j in range(X):
                pkv[l, j, :, i * D:(i + 1) * D] = p[:, j * D:(j + 1) * D]
        for m in (2, 3, 1):
            t = px[m]
            remote(pkv.at[l, t], rkv.at[l, m - 1], qsend.at[l, 1], qrecv.at[l, 1], me_y, t)

        wait_bytes(win_b.at[l], wsem.at[l, 1], "w_win")
        for i in range(CH):
            cols = pl.ds(pl.multiple_of((1 - core) * FH + i * CW, CW), CW)
            fsib[l, i] = jnp.dot(xs[...], win_b[l, :, cols], preferred_element_type=F32).astype(BF16)
            remote(fsib.at[l, i], fsibr.at[l, i], asend.at[l, i], arecv.at[l, i], me_y, sib)
        for i in range(CH):
            cols = pl.ds(pl.multiple_of(core * FH + i * CW, CW), CW)
            fown[i] = jnp.dot(xs[...], win_b[l, :, cols], preferred_element_type=F32)
        for i in range(CH):
            wait_bytes(fsibr.at[l, i], arecv.at[l, i], "w_fs")
            s = fown[i] + fsibr[l, i].astype(F32)
            fown[i] = s
            fcross[l, i] = s.astype(BF16)
            remote(fcross.at[l, i], fcrossr.at[l, i], bsend.at[l, i], brecv.at[l, i], me_y, cross)

        scale = D ** -0.5
        wait_bytes(v_b.at[l], wsem.at[l, 3], "w_v")
        wait_bytes(rq.at[l], qrecv.at[l, 0], "w_q")
        s = pq[l, me_x].astype(F32)
        for d in range(X - 1):
            s = s + rq[l, d].astype(F32)
        q = rope(s.astype(BF16))
        q_b[...] = q
        G = 16
        grow = lax.broadcasted_iota(jnp.int32, (G, S), 0)
        orow = lax.broadcasted_iota(jnp.int32, (G, D), 0)
        pos = lax.broadcasted_iota(jnp.int32, (G, S), 1).astype(F32)

        def scores(i):
            b0 = i * G
            qg = q_b[b0:b0 + G, :]
            acc = jnp.zeros((G, S), F32)
            for j in range(G):
                acc = jnp.where(grow == j, jnp.dot(qg, kt_b[b0 + j], preferred_element_type=F32), acc)
            ln = lenb[b0:b0 + G, :]
            sc = jnp.where(pos < jnp.concatenate([ln] * (S // D), axis=1), acc * scale, -jnp.inf)
            m = jnp.max(sc, axis=1, keepdims=True)
            p = jnp.exp(sc - m)
            m_b[b0:b0 + G, :] = jnp.broadcast_to(m, (G, D))
            d_b[b0:b0 + G, :] = jnp.broadcast_to(jnp.sum(p, axis=1, keepdims=True), (G, D))
            return p.astype(BF16)

        def values(i, p):
            b0 = i * G
            acc = jnp.zeros((G, D), F32)
            for j in range(G):
                acc = jnp.where(orow == j, jnp.dot(p, v_b[l, b0 + j], preferred_element_type=F32), acc)
            of32[b0:b0 + G, :] = acc

        with jax.named_scope("attn"):
            prev = scores(0)
            for i in range(1, B // G):
                cur = scores(i)
                values(i - 1, prev)
                prev = cur
            values(B // G - 1, prev)

        wait_bytes(rkv.at[l], qrecv.at[l, 1], "w_kv")
        s = pkv[l, me_x].astype(F32)
        for d in range(X - 1):
            s = s + rkv[l, d].astype(F32)
        k = rope(s[:, :D].astype(BF16))
        v = s[:, D:].astype(BF16)
        k_out[l] = k
        v_out[l] = v
        sn = jnp.sum(q_b[...].astype(F32) * k.astype(F32), axis=1, keepdims=True) * scale
        m = jnp.maximum(m_b[...], sn)
        al = jnp.exp(m_b[...] - m)
        pn = jnp.exp(sn - m)
        den = d_b[...] * al + pn
        o = of32[...] * al + pn * v.astype(F32)
        obuf[l, me_x] = (o / den).astype(BF16)
        for m in (2, 3, 1):
            t = px[m]
            remote(obuf.at[l, me_x], obuf.at[l, me_x], osend.at[l], orecv.at[l], me_y, t)

        for i in range(CH):
            wait_bytes(fcrossr.at[l, i], brecv.at[l, i], "w_fc")
            s = fown[i] + fcrossr[l, i].astype(F32)
            c = core * CH + i
            fbuf[l, c] = _gelu(s.astype(BF16).astype(F32)).astype(BF16)
            remote(fbuf.at[l, c], fbuf.at[l, c], csend.at[l, i], crecv.at[l, i], me_y, sib)

        wait_bytes(wout_b.at[l], wsem.at[l, 4], "w_wout")

        def f_rows(c):
            return pl.ds(pl.multiple_of(c * CW, CW), CW)

        f = jnp.concatenate([fbuf[l, core * CH + i] for i in range(CH)], axis=1)
        rows = pl.ds(pl.multiple_of(core * FH, FH), FH)
        yacc[...] = jnp.dot(f, wout_b[l, rows, :], preferred_element_type=F32)
        for i in range(CH - 1):
            wait_bytes(fbuf.at[l, i], crecv.at[l, i], "w_fg")
            c = (1 - core) * CH + i
            yacc[...] = yacc[...] + jnp.dot(fbuf[l, c], wout_b[l, f_rows(c), :], preferred_element_type=F32)
        wait_bytes(wo_b.at[l], wsem.at[l, 5], "w_wo")
        wait_bytes(fbuf.at[l, 0], crecv.at[l, CH - 1], "w_fg")
        wait_bytes(obuf.at[l, pl.ds(0, X - 1)], orecv.at[l], "w_og")
        og = jnp.concatenate([obuf[l, j] for j in range(X)], axis=1)
        c = (1 - core) * CH + CH - 1
        near = lax.div(me_y, Y // 2)
        W = Y // 2 * BLK
        for hz, ms in ((1 - near, masks[:Y // 2]), (near, masks[Y // 2:])):
            cols = pl.ds(pl.multiple_of(hz * W, W), W)
            acc = (yacc[:, cols] + jnp.dot(fbuf[l, c], wout_b[l, f_rows(c), cols], preferred_element_type=F32)
                   + jnp.dot(og, wo_b[l, :, cols], preferred_element_type=F32))
            for j in range(Y // 2):
                ybuf[l, hz * (Y // 2) + j] = acc[:, j * BLK:(j + 1) * BLK].astype(BF16)
            for m in ms:
                remote(ybuf.at[l, py[m]], ry.at[l, m - 1], ysend.at[l], yrecv.at[l], py[m], me_x)
        if l + 1 < L:
            transpose_k(l + 1)
        wait_bytes(hbuf.at[l, pl.ds(0, Y - 1)], hsend.at[l])
        wait_bytes(ry.at[l], yrecv.at[l], "w_y")
        y = ybuf[l, me_y].astype(F32)
        for d in range(Y - 1):
            y = y + ry[l, d].astype(F32)
        hcur[...] = (hcur[...].astype(F32) + y.astype(BF16).astype(F32)).astype(BF16)
    h_out[...] = hcur[...]

    for l in range(L):
        wait_bytes(ssbuf.at[l], ssend.at[l])
        wait_bytes(rq.at[l], qsend.at[l, 0])
        wait_bytes(rkv.at[l], qsend.at[l, 1])
        for i in range(CH):
            wait_bytes(fsib.at[l, i], asend.at[l, i])
            wait_bytes(fcross.at[l, i], bsend.at[l, i])
            wait_bytes(fbuf.at[l, i], csend.at[l, i])
        wait_bytes(obuf.at[l, pl.ds(0, X - 1)], osend.at[l])
        wait_bytes(ry.at[l], ysend.at[l])
    wait_bytes(gbuf.at[pl.ds(0, Y - 1)], gsend)


def _finish(h, k, v, h_out, k_out, v_out, sem):
    copies = [pltpu.make_async_copy(a, b, sem.at[i]) for i, (a, b) in enumerate(((k, k_out), (v, v_out), (h, h_out)))]
    for c in copies:
        c.start()
    for c in copies:
        c.wait()


def solution(mesh):
    X = mesh.shape['x']
    Y = mesh.shape['yz']
    act = P(None, ('x', 'yz'))
    w_first = P(None, 'x', 'yz')
    w_second = P(None, 'yz', 'x')
    cache = P(None, None, ('yz', 'x'), None, None)
    new = P(None, None, ('yz', 'x'), None)

    def body(h, g, wq, wk, wv, w_in, wo, w_out, kc, vc, lens):
        B, BLK = h.shape
        L, E, HD = wq.shape
        FL = w_in.shape[2]
        S, D = kc.shape[3], kc.shape[4]
        half = D // 2
        CW = FL // 2 // CH
        kc = kc.reshape(L, B, S, D)
        vc = vc.reshape(L, B, S, D)
        i = np.arange(half, dtype=np.float32)
        inv = np.power(np.float32(10000.0), -i / np.float32(half)).astype(np.float32)
        inv = jnp.asarray(np.concatenate([inv, inv])[None])
        vm = pl.BlockSpec(memory_space=pltpu.VMEM)
        hbm = pl.BlockSpec(memory_space=pl.ANY)
        far = pl.BlockSpec(memory_space=pltpu.HBM)
        N = X * Y
        dma = pltpu.SemaphoreType.DMA
        V = pltpu.VMEM
        scratch = [
            V((L, E, 3 * HD), BF16), V((L, E, FL), BF16), V((L, HD, E), BF16), V((L, FL, E), BF16),
            V((L, B, S, D), BF16), V((L, B, S, D), BF16), V((B, D, S), BF16),
            V((B, BLK), BF16), V((L, Y, B, BLK), BF16), V((L, BLK), BF16), V((Y, L, BLK), BF16),
            V((1, B), jnp.int32), V((1, D), F32),
            V((L, 1, D), F32), V((L, N - Y, 1, D), F32), V((B, Y * BLK), BF16),
            V((B, D), F32), V((B, D), F32), V((B, D), F32),
            V((L, X, B, D), BF16), V((L, X, B, 2 * D), BF16),
            V((L, X - 1, B, D), BF16), V((L, X - 1, B, 2 * D), BF16),
            V((B, D), BF16), V((B, D), F32), V((B, D), F32), V((B, D), F32), V((L, X, B, D), BF16),
            V((L, CH, B, CW), BF16), V((L, CH, B, CW), BF16), V((CH, B, CW), F32),
            V((L, CH, B, CW), BF16), V((L, CH, B, CW), BF16), V((L, 2 * CH, B, CW), BF16),
            V((B, Y * BLK), F32), V((L, Y, B, BLK), BF16), V((L, Y - 1, B, BLK), BF16),
            dma((4,)), dma((L, 6)), dma((L,)), dma((L,)), dma, dma, dma((L,)), dma((L,)), dma((L, 2)), dma((L, 2)),
            dma((L, CH)), dma((L, CH)), dma((L, CH)), dma((L, CH)), dma((L, CH)), dma((L, CH)),
            dma((L,)), dma((L,)), dma((L,)), dma((L,)),
        ]
        shapes = (jax.ShapeDtypeStruct((B, BLK), BF16),
                  jax.ShapeDtypeStruct((L, B, D), BF16),
                  jax.ShapeDtypeStruct((L, B, D), BF16))
        outs = pl.pallas_call(
            functools.partial(_kernel, X, Y, float(BLK * N)),
            out_shape=tuple(V(t.shape, t.dtype) for t in shapes),
            in_specs=[hbm] * 12,
            out_specs=(vm, vm, vm),
            scratch_shapes=scratch,
            compiler_params=pltpu.CompilerParams(
                collective_id=0, has_side_effects=True, vmem_limit_bytes=56 * 1024 * 1024),
            name="decode_step",
        )(h, g, lens.reshape(1, B), inv, wq, wk, wv, w_in, wo, w_out, kc, vc)
        h_new, k_new, v_new = pl.pallas_call(
            _finish, out_shape=shapes, in_specs=[vm] * 3, out_specs=(far, far, far), name="finish",
            scratch_shapes=[dma((3,))],
        )(*[pltpu.with_memory_space_constraint(t, pltpu.VMEM) for t in outs])
        return h_new, k_new.reshape(L, B, 1, D), v_new.reshape(L, B, 1, D)

    return jax.shard_map(
        body, mesh=mesh,
        in_specs=(act, act, w_first, w_first, w_first, w_first, w_second, w_second, cache, cache, P(None)),
        out_specs=(act, new, new), check_vma=False)
```

```python
import functools
import math

import numpy as np

import jax
import jax.numpy as jnp
from jax import lax
from jax.experimental import pallas as pl
from jax.experimental.pallas import tpu as pltpu
from jax.sharding import PartitionSpec as P

EPS = 1e-6
MESH = pl.DeviceIdType.MESH
F32 = jnp.float32
BF16 = jnp.bfloat16
QUARTERS = ((0, 2), (2, 1), (3, 1))
NC = len(QUARTERS)


def _gelu(x):
    return 0.5 * x * (1.0 + jnp.tanh(math.sqrt(2.0 / math.pi) * (x + 0.044715 * (x * x * x))))


def _partner(i, mask):
    bit = 1
    t = i
    while bit <= mask:
        if mask & bit:
            t = t + bit * (1 - 2 * lax.rem(lax.div(i, bit), 2))
        bit *= 2
    return t


def _kernel(X, Y, e_total, h_ref, g_ref, lens_ref, inv_ref, wq, wk, wv, w_in, wo, w_out, kc, vc,
            h_out, k_out, v_out,
            wqkv_b, win_b, wo_b, wout_b, k_b, v_b, kt_b,
            hx, hbuf0, hbuf, lens_b, inv_b, ssown, ssbuf, xs, cos_b, sin_b, lenb,
            pq, pk, pv, rq, rv, rks, kx, rkx, q_b, m_b, d_b, of32, obuf,
            fsib, fsibr, fown, fcross, fcrossr, fbuf, yacc, ybuf, ry,
            isem, wsem, sent, hrecv, srecv, qrecv, arecv, brecv, crecv, orecv, ysend, yrecv):
    me_y = lax.axis_index("yz")
    me_x = lax.axis_index("x")
    N = X * Y
    L = wqkv_b.shape[0]
    B, BLK = h_ref.shape
    S, D = kc.shape[2], kc.shape[3]
    HD = wq.shape[2]
    FL = w_in.shape[2]
    FH = FL // 2
    HW = FH // 2
    CW = FH // 4
    half = D // 2
    core = lax.rem(me_x, 2)
    py = [_partner(me_y, m) for m in range(Y)]
    px = [_partner(me_x, m) for m in range(X)]
    sib, cross = px[1], px[2]
    masks = list(range(Y - 1, 0, -1))
    near = lax.div(me_y, Y // 2)
    total = [0]

    barrier = pltpu.get_barrier_semaphore()
    for m in range(Y - 1, -1, -1):
        for n in range(X - 1, -1, -1):
            if m or n:
                pl.semaphore_signal(barrier, inc=1, device_id=(py[m], px[n]), device_id_type=MESH)

    def remote(src, dst, recv, y, x, send=None):
        if send is None:
            total[0] += math.prod(src.shape) * np.dtype(src.dtype).itemsize
        pltpu.make_async_remote_copy(src, dst, sent if send is None else send, recv,
                                     device_id=(y, x), device_id_type=MESH).start()

    def wait_bytes(ref, sem, name="wait"):
        with jax.named_scope(name):
            pltpu.make_async_copy(ref, ref, sem).wait()

    inputs = [pltpu.make_async_copy(s, d, isem) for s, d in (
        (h_ref, hx.at[pl.ds(0, B)]), (g_ref, hx.at[pl.ds(B, L)]), (lens_ref, lens_b), (inv_ref, inv_b))]
    for c in inputs:
        c.start()

    def load(w, b, l, i, parts=4):
        n = w.shape[1] // parts
        for j in range(parts):
            pltpu.make_async_copy(w.at[l, pl.ds(j * n, n)], b.at[l, pl.ds(j * n, n)], wsem.at[i]).start()

    def load_qkv(l, i):
        for j, w in enumerate((wq, wk, wv)):
            pltpu.make_async_copy(w.at[l], wqkv_b.at[l, :, pl.ds(j * HD, HD)], wsem.at[i]).start()

    def transpose_k(l):
        wait_bytes(k_b.at[l], wsem.at[3 * l], "w_k")

        def step(i, carry):
            for j in range(8):
                kt_b[i * 8 + j] = k_b[l, i * 8 + j].T
            return carry

        with jax.named_scope("kt"):
            lax.fori_loop(0, B // 8, step, 0)

    for c in inputs:
        c.wait()
    load(kc, k_b, 0, 0)
    load_qkv(0, 1)
    load(w_in, win_b, 0, 1)
    load(vc, v_b, 0, 2)
    load(w_out, wout_b, 0, 2)
    load(wo, wo_b, 0, 2, 1)
    for l in range(1, L):
        load(kc, k_b, l, 3)
        load_qkv(l, 4)
        load(w_in, win_b, l, 4)
        load(vc, v_b, l, 4)
        load(w_out, wout_b, l, 4)
        load(wo, wo_b, l, 4, 1)

    row = lax.broadcasted_iota(jnp.int32, (B, D), 0)
    lane = lax.broadcasted_iota(jnp.int32, (B, D), 1)

    def column(r):
        return jnp.sum(jnp.where(row == lane, jnp.broadcast_to(r, (B, D)), 0.0), axis=1, keepdims=True)

    def as_row(c):
        return jnp.sum(jnp.where(row == lane, jnp.broadcast_to(c, (B, D)), 0.0), axis=0, keepdims=True)

    lens_row = jnp.concatenate([lens_b[...].astype(F32), jnp.zeros((1, D - B), F32)], axis=1)
    lens_col = column(lens_row)
    lenb[...] = jnp.broadcast_to(lens_col, (B, D))
    ang = lens_col * inv_b[...]
    cos_b[...] = jnp.cos(ang)
    sn = jnp.sin(ang)
    sin_b[...] = jnp.where(lane < half, -sn, sn)

    def rope(t):
        tf = t.astype(F32)
        return (tf * cos_b[...] + pltpu.roll(tf, half, 1) * sin_b[...]).astype(BF16)

    def send_ss(l, hn):
        hf = hn.astype(F32)
        ssown[l] = as_row(jnp.sum(hf * hf, axis=1, keepdims=True))

    def exchange_h(l, src, dst):
        for m in range(Y - 1, -1, -1):
            for n in range(X - 1, 0, -1):
                remote(ssown.at[l], ssbuf.at[l, m * (X - 1) + n - 1], srecv, py[m], px[n])
        for m in masks:
            remote(src, dst.at[me_y], hrecv, py[m], me_x)

    send_ss(0, hx[0:B])
    hbuf0[me_y] = hx[...]

    with jax.named_scope("w_bar"):
        pl.semaphore_wait(barrier, N - 1)
    exchange_h(0, hx, hbuf0)
    transpose_k(0)

    for l in range(L):
        last = l == L - 1
        hall = hbuf if l else hbuf0
        wait_bytes(hall.at[pl.ds(0, Y - 1)], hrecv, "w_h")
        wait_bytes(ssbuf.at[l], srecv, "w_ss")
        row_ss = jnp.zeros((B, BLK), F32)
        for j in range(Y):
            hf = hall[j, 0:B].astype(F32)
            row_ss = row_ss + hf * hf
        tot = jnp.sum(row_ss, axis=1, keepdims=True) + column(jnp.sum(ssbuf[l], axis=0))
        r = lax.rsqrt(tot / e_total + EPS)
        for j in range(Y):
            gl = hbuf0[j, B + l:B + l + 1].astype(F32)
            xs[:, j * BLK:(j + 1) * BLK] = (hall[j, 0:B].astype(F32) * r * gl).astype(BF16)

        if l == 0:
            wait_bytes(wqkv_b.at[l], wsem.at[1], "w_wqkv")
            wait_bytes(win_b.at[l], wsem.at[1], "w_win")
        else:
            for b in (wqkv_b, win_b, v_b, wout_b, wo_b):
                wait_bytes(b.at[l], wsem.at[4], "w_w1")

        def part(i, dst):
            p = jnp.dot(xs[...], wqkv_b[l, :, i * HD:(i + 1) * HD], preferred_element_type=F32).astype(BF16)
            for j in range(X):
                dst[l, j] = p[:, j * D:(j + 1) * D]

        part(0, pq)
        for m in (2, 3, 1):
            remote(pq.at[l, px[m]], rq.at[l, m - 1], qrecv.at[0], me_y, px[m])
        part(1, pk)
        for i, t in enumerate((px[3], sib)):
            remote(pk.at[l, t], rks.at[l, i], qrecv.at[1], me_y, sib)
        part(2, pv)
        for m in (2, 3, 1):
            remote(pv.at[l, px[m]], rv.at[l, m - 1], qrecv.at[2], me_y, px[m])


        def f_part(c, i):
            cols = pl.ds(pl.multiple_of(c * FH + i * HW, HW), HW)
            return jnp.dot(xs[...], win_b[l, :, cols], preferred_element_type=F32)

        def f_sib(i):
            fsib[l, i] = f_part(1 - core, i).astype(BF16)
            remote(fsib.at[l, i], fsibr.at[l, i], arecv.at[i], me_y, sib)

        def f_add(i):
            wait_bytes(fsibr.at[l, i], arecv.at[i], "w_fs")
            s = fown[i] + fsibr[l, i].astype(F32)
            fown[i] = s
            for j in range(2):
                fcross[l, 2 * i + j] = s[:, j * CW:(j + 1) * CW].astype(BF16)
            for c, (q0, nq) in enumerate(QUARTERS):
                if q0 // 2 == i:
                    qs = pl.ds(q0, nq)
                    remote(fcross.at[l, qs], fcrossr.at[l, qs], brecv.at[c], me_y, cross)

        f_sib(0)
        fown[0] = f_part(core, 0)
        wait_bytes(rks.at[l], qrecv.at[1], "w_ks")
        kx[l] = (pk[l, cross].astype(F32) + rks[l, 0].astype(F32)).astype(BF16)
        remote(kx.at[l], rkx.at[l], qrecv.at[3], me_y, cross)
        f_sib(1)
        f_add(0)
        fown[1] = f_part(core, 1)
        f_add(1)

        scale = D ** -0.5
        if l == 0:
            for b in (v_b, wout_b, wo_b):
                wait_bytes(b.at[l], wsem.at[2], "w_v")
        wait_bytes(rq.at[l], qrecv.at[0], "w_q")
        s = pq[l, me_x].astype(F32)
        for d in range(X - 1):
            s = s + rq[l, d].astype(F32)
        q = rope(s.astype(BF16))
        q_b[...] = q
        G = 16
        grow = lax.broadcasted_iota(jnp.int32, (G, S), 0)
        orow = lax.broadcasted_iota(jnp.int32, (G, D), 0)
        pos = lax.broadcasted_iota(jnp.int32, (G, S), 1).astype(F32)

        def scores(i):
            b0 = i * G
            qg = q_b[b0:b0 + G, :]
            acc = jnp.zeros((G, S), F32)
            for j in range(G):
                acc = jnp.where(grow == j, jnp.dot(qg, kt_b[b0 + j], preferred_element_type=F32), acc)
            ln = lenb[b0:b0 + G, :]
            sc = jnp.where(pos < jnp.concatenate([ln] * (S // D), axis=1), acc * scale, -jnp.inf)
            m = jnp.max(sc, axis=1, keepdims=True)
            p = jnp.exp(sc - m)
            m_b[b0:b0 + G, :] = jnp.broadcast_to(m, (G, D))
            d_b[b0:b0 + G, :] = jnp.broadcast_to(jnp.sum(p, axis=1, keepdims=True), (G, D))
            return p.astype(BF16)

        def values(i, p):
            b0 = i * G
            acc = jnp.zeros((G, D), F32)
            for j in range(G):
                acc = jnp.where(orow == j, jnp.dot(p, v_b[l, b0 + j], preferred_element_type=F32), acc)
            of32[b0:b0 + G, :] = acc

        with jax.named_scope("attn"):
            prev = scores(0)
            for i in range(1, B // G):
                cur = scores(i)
                values(i - 1, prev)
                prev = cur
            values(B // G - 1, prev)

        wait_bytes(rv.at[l], qrecv.at[2], "w_nv")
        wait_bytes(rkx.at[l], qrecv.at[3], "w_nk")
        s = pv[l, me_x].astype(F32)
        for d in range(X - 1):
            s = s + rv[l, d].astype(F32)
        v = s.astype(BF16)
        k = rope((pk[l, me_x].astype(F32) + rks[l, 1].astype(F32) + rkx[l].astype(F32)).astype(BF16))
        sn = jnp.sum(q_b[...].astype(F32) * k.astype(F32), axis=1, keepdims=True) * scale
        m = jnp.maximum(m_b[...], sn)
        al = jnp.exp(m_b[...] - m)
        pn = jnp.exp(sn - m)
        den = d_b[...] * al + pn
        o = of32[...] * al + pn * v.astype(F32)
        obuf[l, me_x] = (o / den).astype(BF16)
        for m in (2, 3, 1):
            remote(obuf.at[l, me_x], obuf.at[l, me_x], orecv, me_y, px[m])
        k_out[l] = k
        v_out[l] = v

        def f_dot(q0, nq, cols):
            f = jnp.concatenate([fbuf[l, q0 + i] for i in range(nq)], axis=1)
            rows = pl.ds(pl.multiple_of(q0 * CW, CW), nq * CW)
            return jnp.dot(f, wout_b[l, rows, cols], preferred_element_type=F32)

        mine, other = core * 4, (1 - core) * 4
        everything = slice(None)
        for c, (q0, nq) in enumerate(QUARTERS):
            wait_bytes(fcrossr.at[l, pl.ds(q0, nq)], brecv.at[c], "w_fc")
            for i in range(q0, q0 + nq):
                s = fown[i // 2, :, (i % 2) * CW:(i % 2 + 1) * CW] + fcrossr[l, i].astype(F32)
                fbuf[l, mine + i] = _gelu(s.astype(BF16).astype(F32)).astype(BF16)
            qs = pl.ds(mine + q0, nq)
            remote(fbuf.at[l, qs], fbuf.at[l, qs], crecv.at[c], me_y, sib)
            if c == 0:
                yacc[...] = f_dot(mine + q0, nq, everything)
            elif c == 1:
                yacc[...] = yacc[...] + f_dot(mine + q0, nq, everything)
            else:
                p0, np_ = QUARTERS[0]
                wait_bytes(fbuf.at[l, pl.ds(p0, np_)], crecv.at[0], "w_fg")
                yacc[...] = yacc[...] + (f_dot(mine + q0, nq, everything) + f_dot(other + p0, np_, everything))
        p0, np_ = QUARTERS[1]
        wait_bytes(fbuf.at[l, pl.ds(p0, np_)], crecv.at[1], "w_fg")
        wait_bytes(obuf.at[l, pl.ds(0, X - 1)], orecv, "w_og")
        og = jnp.concatenate([obuf[l, j] for j in range(X)], axis=1)
        yacc[...] = yacc[...] + (f_dot(other + p0, np_, everything)
                                 + jnp.dot(og, wo_b[l], preferred_element_type=F32))
        p0, np_ = QUARTERS[2]
        wait_bytes(fbuf.at[l, pl.ds(p0, np_)], crecv.at[2], "w_fg")
        W = Y // 2 * BLK
        for hz, ms in ((1 - near, masks[:Y // 2]), (near, masks[Y // 2:])):
            cols = pl.ds(pl.multiple_of(hz * W, W), W)
            acc = yacc[:, cols] + f_dot(other + p0, np_, cols)
            for j in range(Y // 2):
                ybuf[l, hz * (Y // 2) + j] = acc[:, j * BLK:(j + 1) * BLK].astype(BF16)
            for m in ms:
                remote(ybuf.at[l, py[m]], ry.at[l, m - 1], yrecv, py[m], me_x, ysend if last else None)
        if last:
            n = total[0]
            big = S * D * 2
            wait_bytes(k_b.at[0, pl.ds(0, n // big)], sent)
            if n % big:
                wait_bytes(k_b.at[0, 0, pl.ds(0, n % big // (2 * D))], sent)
            wait_bytes(ry.at[l], ysend)
        else:
            transpose_k(l + 1)
        wait_bytes(ry.at[l], yrecv, "w_y")
        y = ybuf[l, me_y].astype(F32)
        for d in range(Y - 1):
            y = y + ry[l, d].astype(F32)
        hn = (hall[me_y, 0:B].astype(F32) + y.astype(BF16).astype(F32)).astype(BF16)
        if last:
            h_out[...] = hn
        else:
            send_ss(l + 1, hn)
            hbuf[me_y] = hn
            exchange_h(l + 1, hbuf.at[me_y], hbuf)


def _finish(h, k, v, h_out, k_out, v_out, sem):
    copies = [pltpu.make_async_copy(a, b, sem.at[i]) for i, (a, b) in enumerate(((k, k_out), (v, v_out), (h, h_out)))]
    for c in copies:
        c.start()
    for c in copies:
        c.wait()


def solution(mesh):
    X = mesh.shape['x']
    Y = mesh.shape['yz']
    act = P(None, ('x', 'yz'))
    w_first = P(None, 'x', 'yz')
    w_second = P(None, 'yz', 'x')
    cache = P(None, None, ('yz', 'x'), None, None)
    new = P(None, None, ('yz', 'x'), None)

    def body(h, g, wq, wk, wv, w_in, wo, w_out, kc, vc, lens):
        B, BLK = h.shape
        L, E, HD = wq.shape
        FL = w_in.shape[2]
        S, D = kc.shape[3], kc.shape[4]
        half = D // 2
        CW = FL // 8
        kc = kc.reshape(L, B, S, D)
        vc = vc.reshape(L, B, S, D)
        i = np.arange(half, dtype=np.float32)
        inv = np.power(np.float32(10000.0), -i / np.float32(half)).astype(np.float32)
        inv = jnp.asarray(np.concatenate([inv, inv])[None])
        vm = pl.BlockSpec(memory_space=pltpu.VMEM)
        hbm = pl.BlockSpec(memory_space=pl.ANY)
        far = pl.BlockSpec(memory_space=pltpu.HBM)
        N = X * Y
        dma = pltpu.SemaphoreType.DMA
        V = pltpu.VMEM
        scratch = [
            V((L, E, 3 * HD), BF16), V((L, E, FL), BF16), V((L, HD, E), BF16), V((L, FL, E), BF16),
            V((L, B, S, D), BF16), V((L, B, S, D), BF16), V((B, D, S), BF16),
            V((B + 8, BLK), BF16), V((Y, B + 8, BLK), BF16), V((Y, B, BLK), BF16),
            V((1, B), jnp.int32), V((1, D), F32),
            V((L, 1, D), F32), V((L, N - Y, 1, D), F32), V((B, Y * BLK), BF16),
            V((B, D), F32), V((B, D), F32), V((B, D), F32),
            V((L, X, B, D), BF16), V((L, X, B, D), BF16), V((L, X, B, D), BF16),
            V((L, X - 1, B, D), BF16), V((L, X - 1, B, D), BF16), V((L, 2, B, D), BF16),
            V((L, B, D), BF16), V((L, B, D), BF16),
            V((B, D), BF16), V((B, D), F32), V((B, D), F32), V((B, D), F32), V((L, X, B, D), BF16),
            V((L, 2, B, 2 * CW), BF16), V((L, 2, B, 2 * CW), BF16), V((2, B, 2 * CW), F32),
            V((L, 4, B, CW), BF16), V((L, 4, B, CW), BF16), V((L, 8, B, CW), BF16),
            V((B, Y * BLK), F32), V((L, Y, B, BLK), BF16), V((L, Y - 1, B, BLK), BF16),
            dma, dma((5,)), dma, dma, dma, dma((4,)), dma((2,)), dma((NC,)), dma((NC,)), dma, dma, dma,
        ]
        shapes = (jax.ShapeDtypeStruct((B, BLK), BF16),
                  jax.ShapeDtypeStruct((L, B, D), BF16),
                  jax.ShapeDtypeStruct((L, B, D), BF16))
        outs = pl.pallas_call(
            functools.partial(_kernel, X, Y, float(BLK * N)),
            out_shape=tuple(V(t.shape, t.dtype) for t in shapes),
            in_specs=[hbm] * 12,
            out_specs=(vm, vm, vm),
            scratch_shapes=scratch,
            compiler_params=pltpu.CompilerParams(
                collective_id=0, has_side_effects=True, vmem_limit_bytes=56 * 1024 * 1024),
            name="decode_step",
        )(h, g, lens.reshape(1, B), inv, wq, wk, wv, w_in, wo, w_out, kc, vc)
        h_new, k_new, v_new = pl.pallas_call(
            _finish, out_shape=shapes, in_specs=[vm] * 3, out_specs=(far, far, far), name="finish",
            scratch_shapes=[dma((3,))],
        )(*[pltpu.with_memory_space_constraint(t, pltpu.VMEM) for t in outs])
        return h_new, k_new.reshape(L, B, 1, D), v_new.reshape(L, B, 1, D)

    return jax.shard_map(
        body, mesh=mesh,
        in_specs=(act, act, w_first, w_first, w_first, w_first, w_second, w_second, cache, cache, P(None)),
        out_specs=(act, new, new), check_vma=False)
```

```python
import functools
import math

import numpy as np

import jax
import jax.numpy as jnp
from jax import lax
from jax.experimental import pallas as pl
from jax.experimental.pallas import tpu as pltpu
from jax.sharding import PartitionSpec as P

EPS = 1e-6
MESH = pl.DeviceIdType.MESH
F32 = jnp.float32
BF16 = jnp.bfloat16
QUARTERS = ((0, 2), (2, 1), (3, 1))
NC = len(QUARTERS)
UP, DOWN = 2.0 ** 18, 2.0 ** -18


def _gelu(x):
    return 0.5 * x * (1.0 + jnp.tanh(math.sqrt(2.0 / math.pi) * (x + 0.044715 * (x * x * x))))


def _partner(i, mask):
    bit = 1
    t = i
    while bit <= mask:
        if mask & bit:
            t = t + bit * (1 - 2 * lax.rem(lax.div(i, bit), 2))
        bit *= 2
    return t


def _kernel(X, Y, h_ref, g_ref, lens_ref, inv_ref, wq, wk, wv, w_in, wo, w_out, kc, vc,
            h_out, k_out, v_out,
            wqkv_b, win_b, wo_b, wout_b, k_b, v_b, kt_b,
            hx, hbuf0, hbuf, lens_b, inv_b, mown, mrow, xs, cos_b, sin_b, lenb,
            pq, pk, pv, rq, rv, rks, kx, rkx, q_b, m_b, d_b, of32, obuf,
            fsib, fsibr, fown, fcross, fcrossr, fbuf, yacc, ybuf, ry,
            isem, wsem, sent, hrecv, mrecv, qrecv, arecv, brecv, crecv, orecv, ysend, yrecv):
    me_y = lax.axis_index("yz")
    me_x = lax.axis_index("x")
    L = wqkv_b.shape[0]
    B, BLK = h_ref.shape
    S, D = kc.shape[2], kc.shape[3]
    HD = wq.shape[2]
    FL = w_in.shape[2]
    FH = FL // 2
    HW = FH // 2
    CW = FH // 4
    half = D // 2
    core = lax.rem(me_x, 2)
    py = [_partner(me_y, m) for m in range(Y)]
    px = [_partner(me_x, m) for m in range(X)]
    sib, cross = px[1], px[2]
    masks = list(range(Y - 1, 0, -1))
    near = lax.div(me_y, Y // 2)
    total = [0]

    barrier = pltpu.get_barrier_semaphore()
    for m in masks:
        pl.semaphore_signal(barrier, inc=1, device_id=(py[m], me_x), device_id_type=MESH)
    for n in range(X - 1, 0, -1):
        pl.semaphore_signal(barrier, inc=1, device_id=(me_y, px[n]), device_id_type=MESH)

    def remote(src, dst, recv, y, x, send=None):
        if send is None:
            total[0] += math.prod(src.shape) * np.dtype(src.dtype).itemsize
        pltpu.make_async_remote_copy(src, dst, sent if send is None else send, recv,
                                     device_id=(y, x), device_id_type=MESH).start()

    def wait_bytes(ref, sem, name="wait"):
        with jax.named_scope(name):
            pltpu.make_async_copy(ref, ref, sem).wait()

    inputs = [pltpu.make_async_copy(s, d, isem) for s, d in (
        (h_ref, hx.at[pl.ds(0, B)]), (g_ref, hx.at[pl.ds(B, L)]), (lens_ref, lens_b), (inv_ref, inv_b))]
    for c in inputs:
        c.start()

    def load(w, b, l, i, parts=4):
        n = w.shape[1] // parts
        for j in range(parts):
            pltpu.make_async_copy(w.at[l, pl.ds(j * n, n)], b.at[l, pl.ds(j * n, n)], wsem.at[i]).start()

    def load_qkv(l, i):
        for j, w in enumerate((wq, wk, wv)):
            pltpu.make_async_copy(w.at[l], wqkv_b.at[l, :, pl.ds(j * HD, HD)], wsem.at[i]).start()

    def transpose_k(l):
        wait_bytes(k_b.at[l], wsem.at[3 * l], "w_k")

        def step(i, carry):
            for j in range(8):
                kt_b[i * 8 + j] = k_b[l, i * 8 + j].T
            return carry

        with jax.named_scope("kt"):
            lax.fori_loop(0, B // 8, step, 0)

    for c in inputs:
        c.wait()
    load(kc, k_b, 0, 0)
    load_qkv(0, 1)
    load(w_in, win_b, 0, 1)
    load(vc, v_b, 0, 2)
    load(w_out, wout_b, 0, 2)
    load(wo, wo_b, 0, 2, 1)
    for l in range(1, L):
        load(kc, k_b, l, 3)
        load_qkv(l, 4)
        load(w_in, win_b, l, 4)
        load(vc, v_b, l, 4)
        load(w_out, wout_b, l, 4)
        load(wo, wo_b, l, 4, 1)

    row = lax.broadcasted_iota(jnp.int32, (B, D), 0)
    lane = lax.broadcasted_iota(jnp.int32, (B, D), 1)

    def column(r):
        return jnp.sum(jnp.where(row == lane, jnp.broadcast_to(r, (B, D)), 0.0), axis=1, keepdims=True)

    def as_row(c):
        return jnp.sum(jnp.where(row == lane, jnp.broadcast_to(c, (B, D)), 0.0), axis=0, keepdims=True)

    lens_row = jnp.concatenate([lens_b[...].astype(F32), jnp.zeros((1, D - B), F32)], axis=1)
    lens_col = column(lens_row)
    lenb[...] = jnp.broadcast_to(lens_col, (B, D))
    ang = lens_col * inv_b[...]
    cos_b[...] = jnp.cos(ang)
    sn = jnp.sin(ang)
    sin_b[...] = jnp.where(lane < half, -sn, sn)

    def rope(t):
        tf = t.astype(F32)
        return (tf * cos_b[...] + pltpu.roll(tf, half, 1) * sin_b[...]).astype(BF16)

    def exchange_h(src, dst):
        for m in masks:
            remote(src, dst.at[me_y], hrecv, py[m], me_x)

    def rms(ss, n):
        return jnp.minimum(jnp.sqrt(ss / n + EPS), 1e38)

    lane1 = lax.broadcasted_iota(jnp.int32, (1, D), 1)
    NX = Y * BLK

    hbuf0[me_y] = hx[...]

    with jax.named_scope("w_bar"):
        pl.semaphore_wait(barrier, X + Y - 2)
    exchange_h(hx, hbuf0)
    transpose_k(0)

    for l in range(L):
        last = l == L - 1
        hall = hbuf if l else hbuf0
        wait_bytes(hall.at[pl.ds(0, Y - 1)], hrecv, "w_h")
        row_ss = jnp.zeros((B, BLK), F32)
        gmax = jnp.zeros((1, BLK), F32)
        for j in range(Y):
            hf = hall[j, 0:B].astype(F32)
            row_ss = row_ss + hf * hf
            gmax = jnp.maximum(gmax, jnp.abs(hbuf0[j, B + l:B + l + 1].astype(F32)))
        ss = jnp.sum(row_ss, axis=1, keepdims=True)
        G = jnp.maximum(jnp.max(gmax, axis=1, keepdims=True), 2.0 ** -100)
        mown[l] = jnp.where(lane1 == B, G, as_row(ss))
        for m in (1, 2, 3):
            remote(mown.at[l], mrow.at[l, m - 1], mrecv.at[0 if m == 1 else 1], me_y, px[m])
        sx = lax.rsqrt(ss / NX + EPS)
        for j in range(Y):
            gl = (hbuf0[j, B + l:B + l + 1].astype(F32) / G) * DOWN
            xs[:, j * BLK:(j + 1) * BLK] = (hall[j, 0:B].astype(F32) * sx * gl).astype(BF16)

        if l == 0:
            wait_bytes(wqkv_b.at[l], wsem.at[1], "w_wqkv")
            wait_bytes(win_b.at[l], wsem.at[1], "w_win")
        else:
            for b in (wqkv_b, win_b, v_b, wout_b, wo_b):
                wait_bytes(b.at[l], wsem.at[4], "w_w1")

        def part(i, dst):
            p = jnp.dot(xs[...], wqkv_b[l, :, i * HD:(i + 1) * HD], preferred_element_type=F32).astype(BF16)
            for j in range(X):
                dst[l, j] = p[:, j * D:(j + 1) * D]

        part(0, pq)
        for m in (2, 3, 1):
            remote(pq.at[l, px[m]], rq.at[l, m - 1], qrecv.at[0], me_y, px[m])
        part(1, pk)
        for i, t in enumerate((px[3], sib)):
            remote(pk.at[l, t], rks.at[l, i], qrecv.at[1], me_y, sib)
        part(2, pv)
        for m in (2, 3, 1):
            remote(pv.at[l, px[m]], rv.at[l, m - 1], qrecv.at[2], me_y, px[m])


        def f_part(c, i):
            cols = pl.ds(pl.multiple_of(c * FH + i * HW, HW), HW)
            return jnp.dot(xs[...], win_b[l, :, cols], preferred_element_type=F32)

        def f_sib(i):
            fsib[l, i] = f_part(1 - core, i).astype(BF16)
            remote(fsib.at[l, i], fsibr.at[l, i], arecv.at[i], me_y, sib)

        def f_add(i):
            wait_bytes(fsibr.at[l, i], arecv.at[i], "w_fs")
            s = fown[i] * w_own + fsibr[l, i].astype(F32) * w_sib
            fown[i] = s
            for j in range(2):
                fcross[l, 2 * i + j] = s[:, j * CW:(j + 1) * CW].astype(BF16)
            for c, (q0, nq) in enumerate(QUARTERS):
                if q0 // 2 == i:
                    qs = pl.ds(q0, nq)
                    remote(fcross.at[l, qs], fcrossr.at[l, qs], brecv.at[l, c], me_y, cross)

        f_sib(0)
        fown[0] = f_part(core, 0)
        wait_bytes(mrow.at[l, 0], mrecv.at[0], "w_ms")
        ss1, G1 = column(mrow[l, 0]), mrow[l, 0, :, B:B + 1]
        ssc, Gc = ss + ss1, jnp.maximum(G, G1)
        sc_ = lax.rsqrt(ssc / (2 * NX) + EPS)
        w_own = sc_ * rms(ss, NX) * (G / Gc)
        w_sib = sc_ * rms(ss1, NX) * (G1 / Gc)
        wait_bytes(rks.at[l], qrecv.at[1], "w_ks")
        kx[l] = (pk[l, cross].astype(F32) * w_own + rks[l, 0].astype(F32) * w_sib).astype(BF16)
        remote(kx.at[l], rkx.at[l], qrecv.at[3], me_y, cross)
        f_sib(1)
        f_add(0)
        fown[1] = f_part(core, 1)
        f_add(1)

        scale = D ** -0.5
        if l == 0:
            for b in (v_b, wout_b, wo_b):
                wait_bytes(b.at[l], wsem.at[2], "w_v")
        wait_bytes(mrow.at[l, pl.ds(1, 2)], mrecv.at[1], "w_m")
        ss2, G2 = column(mrow[l, 1]), mrow[l, 1, :, B:B + 1]
        ss3, G3 = column(mrow[l, 2]), mrow[l, 2, :, B:B + 1]
        ssd, Gd = ss2 + ss3, jnp.maximum(G2, G3)
        r = lax.rsqrt((ssc + ssd) / (4 * NX) + EPS)
        rows4 = [(r * rms(a, NX), b) for a, b in ((ss, G), (ss1, G1), (ss2, G2), (ss3, G3))]
        fc, fd = r * rms(ssc, 2 * NX), r * rms(ssd, 2 * NX)

        def joined(p, got):
            s = (p.astype(F32) * rows4[0][0]) * rows4[0][1]
            for d in range(X - 1):
                s = s + (got[d].astype(F32) * rows4[d + 1][0]) * rows4[d + 1][1]
            return (s * UP).astype(BF16)

        def chips(mine, theirs):
            return (((mine * fc) * Gc + (theirs * fd) * Gd) * UP).astype(BF16)

        wait_bytes(rq.at[l], qrecv.at[0], "w_q")
        q = rope(joined(pq[l, me_x], rq[l]))
        q_b[...] = q
        GB = 16
        grow = lax.broadcasted_iota(jnp.int32, (GB, S), 0)
        orow = lax.broadcasted_iota(jnp.int32, (GB, D), 0)
        pos = lax.broadcasted_iota(jnp.int32, (GB, S), 1).astype(F32)

        def scores(i):
            b0 = i * GB
            qg = q_b[b0:b0 + GB, :]
            acc = jnp.zeros((GB, S), F32)
            for j in range(GB):
                acc = jnp.where(grow == j, jnp.dot(qg, kt_b[b0 + j], preferred_element_type=F32), acc)
            ln = lenb[b0:b0 + GB, :]
            sc = jnp.where(pos < jnp.concatenate([ln] * (S // D), axis=1), acc * scale, -jnp.inf)
            m = jnp.max(sc, axis=1, keepdims=True)
            p = jnp.exp(sc - m)
            m_b[b0:b0 + GB, :] = jnp.broadcast_to(m, (GB, D))
            d_b[b0:b0 + GB, :] = jnp.broadcast_to(jnp.sum(p, axis=1, keepdims=True), (GB, D))
            return p.astype(BF16)

        def values(i, p):
            b0 = i * GB
            acc = jnp.zeros((GB, D), F32)
            for j in range(GB):
                acc = jnp.where(orow == j, jnp.dot(p, v_b[l, b0 + j], preferred_element_type=F32), acc)
            of32[b0:b0 + GB, :] = acc

        with jax.named_scope("attn"):
            prev = scores(0)
            for i in range(1, B // GB):
                cur = scores(i)
                values(i - 1, prev)
                prev = cur
            values(B // GB - 1, prev)

        wait_bytes(rv.at[l], qrecv.at[2], "w_nv")
        wait_bytes(rkx.at[l], qrecv.at[3], "w_nk")
        v = joined(pv[l, me_x], rv[l])
        k = rope(chips(pk[l, me_x].astype(F32) * w_own + rks[l, 1].astype(F32) * w_sib, rkx[l].astype(F32)))
        sn = jnp.sum(q_b[...].astype(F32) * k.astype(F32), axis=1, keepdims=True) * scale
        m = jnp.maximum(m_b[...], sn)
        al = jnp.exp(m_b[...] - m)
        pn = jnp.exp(sn - m)
        den = d_b[...] * al + pn
        o = of32[...] * al + pn * v.astype(F32)
        obuf[l, me_x] = (o / den).astype(BF16)
        for m in (2, 3, 1):
            remote(obuf.at[l, me_x], obuf.at[l, me_x], orecv, me_y, px[m])
        k_out[l] = k
        v_out[l] = v

        def f_dot(q0, nq, cols):
            f = jnp.concatenate([fbuf[l, q0 + i] for i in range(nq)], axis=1)
            rows = pl.ds(pl.multiple_of(q0 * CW, CW), nq * CW)
            return jnp.dot(f, wout_b[l, rows, cols], preferred_element_type=F32)

        mine, other = core * 4, (1 - core) * 4
        everything = slice(None)
        for c, (q0, nq) in enumerate(QUARTERS):
            wait_bytes(fcrossr.at[l, pl.ds(q0, nq)], brecv.at[l, c], "w_fc")
            for i in range(q0, q0 + nq):
                u = chips(fown[i // 2, :, (i % 2) * CW:(i % 2 + 1) * CW], fcrossr[l, i].astype(F32))
                fbuf[l, mine + i] = _gelu(u.astype(F32)).astype(BF16)
            qs = pl.ds(mine + q0, nq)
            remote(fbuf.at[l, qs], fbuf.at[l, qs], crecv.at[c], me_y, sib)
            if c == 0:
                yacc[...] = f_dot(mine + q0, nq, everything)
            elif c == 1:
                yacc[...] = yacc[...] + f_dot(mine + q0, nq, everything)
            else:
                p0, np_ = QUARTERS[0]
                wait_bytes(fbuf.at[l, pl.ds(p0, np_)], crecv.at[0], "w_fg")
                yacc[...] = yacc[...] + (f_dot(mine + q0, nq, everything) + f_dot(other + p0, np_, everything))
        p0, np_ = QUARTERS[1]
        wait_bytes(fbuf.at[l, pl.ds(p0, np_)], crecv.at[1], "w_fg")
        wait_bytes(obuf.at[l, pl.ds(0, X - 1)], orecv, "w_og")
        og = jnp.concatenate([obuf[l, j] for j in range(X)], axis=1)
        yacc[...] = yacc[...] + (f_dot(other + p0, np_, everything)
                                 + jnp.dot(og, wo_b[l], preferred_element_type=F32))
        p0, np_ = QUARTERS[2]
        wait_bytes(fbuf.at[l, pl.ds(p0, np_)], crecv.at[2], "w_fg")
        W = Y // 2 * BLK
        for hz, ms in ((1 - near, masks[:Y // 2]), (near, masks[Y // 2:])):
            cols = pl.ds(pl.multiple_of(hz * W, W), W)
            acc = yacc[:, cols] + f_dot(other + p0, np_, cols)
            for j in range(Y // 2):
                ybuf[l, hz * (Y // 2) + j] = acc[:, j * BLK:(j + 1) * BLK].astype(BF16)
            for m in ms:
                remote(ybuf.at[l, py[m]], ry.at[l, m - 1], yrecv, py[m], me_x, ysend if last else None)
        if last:
            n = total[0]
            big = S * D * 2
            wait_bytes(k_b.at[0, pl.ds(0, n // big)], sent)
            if n % big:
                wait_bytes(k_b.at[0, 0, pl.ds(0, n % big // (2 * D))], sent)
            wait_bytes(ry.at[l], ysend)
        else:
            transpose_k(l + 1)
        wait_bytes(ry.at[l], yrecv, "w_y")
        y = ybuf[l, me_y].astype(F32)
        for d in range(Y - 1):
            y = y + ry[l, d].astype(F32)
        hn = (hall[me_y, 0:B].astype(F32) + y.astype(BF16).astype(F32)).astype(BF16)
        if last:
            h_out[...] = hn
        else:
            hbuf[me_y] = hn
            exchange_h(hbuf.at[me_y], hbuf)


def _finish(h, k, v, h_out, k_out, v_out, sem):
    copies = [pltpu.make_async_copy(a, b, sem.at[i]) for i, (a, b) in enumerate(((k, k_out), (v, v_out), (h, h_out)))]
    for c in copies:
        c.start()
    for c in copies:
        c.wait()


def solution(mesh):
    X = mesh.shape['x']
    Y = mesh.shape['yz']
    act = P(None, ('x', 'yz'))
    w_first = P(None, 'x', 'yz')
    w_second = P(None, 'yz', 'x')
    cache = P(None, None, ('yz', 'x'), None, None)
    new = P(None, None, ('yz', 'x'), None)

    def body(h, g, wq, wk, wv, w_in, wo, w_out, kc, vc, lens):
        B, BLK = h.shape
        L, E, HD = wq.shape
        FL = w_in.shape[2]
        S, D = kc.shape[3], kc.shape[4]
        half = D // 2
        CW = FL // 8
        kc = kc.reshape(L, B, S, D)
        vc = vc.reshape(L, B, S, D)
        i = np.arange(half, dtype=np.float32)
        inv = np.power(np.float32(10000.0), -i / np.float32(half)).astype(np.float32)
        inv = jnp.asarray(np.concatenate([inv, inv])[None])
        vm = pl.BlockSpec(memory_space=pltpu.VMEM)
        hbm = pl.BlockSpec(memory_space=pl.ANY)
        far = pl.BlockSpec(memory_space=pltpu.HBM)
        dma = pltpu.SemaphoreType.DMA
        V = pltpu.VMEM
        scratch = [
            V((L, E, 3 * HD), BF16), V((L, E, FL), BF16), V((L, HD, E), BF16), V((L, FL, E), BF16),
            V((L, B, S, D), BF16), V((L, B, S, D), BF16), V((B, D, S), BF16),
            V((B + 8, BLK), BF16), V((Y, B + 8, BLK), BF16), V((Y, B, BLK), BF16),
            V((1, B), jnp.int32), V((1, D), F32),
            V((L, 1, D), F32), V((L, X - 1, 1, D), F32), V((B, Y * BLK), BF16),
            V((B, D), F32), V((B, D), F32), V((B, D), F32),
            V((L, X, B, D), BF16), V((L, X, B, D), BF16), V((L, X, B, D), BF16),
            V((L, X - 1, B, D), BF16), V((L, X - 1, B, D), BF16), V((L, 2, B, D), BF16),
            V((L, B, D), BF16), V((L, B, D), BF16),
            V((B, D), BF16), V((B, D), F32), V((B, D), F32), V((B, D), F32), V((L, X, B, D), BF16),
            V((L, 2, B, 2 * CW), BF16), V((L, 2, B, 2 * CW), BF16), V((2, B, 2 * CW), F32),
            V((L, 4, B, CW), BF16), V((L, 4, B, CW), BF16), V((L, 8, B, CW), BF16),
            V((B, Y * BLK), F32), V((L, Y, B, BLK), BF16), V((L, Y - 1, B, BLK), BF16),
            dma, dma((5,)), dma, dma, dma((2,)), dma((4,)), dma((2,)), dma((L, NC)), dma((NC,)), dma, dma, dma,
        ]
        shapes = (jax.ShapeDtypeStruct((B, BLK), BF16),
                  jax.ShapeDtypeStruct((L, B, D), BF16),
                  jax.ShapeDtypeStruct((L, B, D), BF16))
        outs = pl.pallas_call(
            functools.partial(_kernel, X, Y),
            out_shape=tuple(V(t.shape, t.dtype) for t in shapes),
            in_specs=[hbm] * 12,
            out_specs=(vm, vm, vm),
            scratch_shapes=scratch,
            compiler_params=pltpu.CompilerParams(
                collective_id=0, has_side_effects=True, vmem_limit_bytes=56 * 1024 * 1024),
            name="decode_step",
        )(h, g, lens.reshape(1, B), inv, wq, wk, wv, w_in, wo, w_out, kc, vc)
        h_new, k_new, v_new = pl.pallas_call(
            _finish, out_shape=shapes, in_specs=[vm] * 3, out_specs=(far, far, far), name="finish",
            scratch_shapes=[dma((3,))],
        )(*[pltpu.with_memory_space_constraint(t, pltpu.VMEM) for t in outs])
        return h_new, k_new.reshape(L, B, 1, D), v_new.reshape(L, B, 1, D)

    return jax.shard_map(
        body, mesh=mesh,
        in_specs=(act, act, w_first, w_first, w_first, w_first, w_second, w_second, cache, cache, P(None)),
        out_specs=(act, new, new), check_vma=False)
```

```python
import functools
import math

import numpy as np

import jax
import jax.numpy as jnp
from jax import lax
from jax.experimental import pallas as pl
from jax.experimental.pallas import tpu as pltpu
from jax.sharding import PartitionSpec as P

EPS = 1e-6
MESH = pl.DeviceIdType.MESH
F32 = jnp.float32
BF16 = jnp.bfloat16
QUARTERS = ((0, 2), (2, 1), (3, 1))
NC = len(QUARTERS)
UP, DOWN = 2.0 ** 18, 2.0 ** -18


def _gelu(x):
    return 0.5 * x * (1.0 + jnp.tanh(math.sqrt(2.0 / math.pi) * (x + 0.044715 * (x * x * x))))


def _partner(i, mask):
    bit = 1
    t = i
    while bit <= mask:
        if mask & bit:
            t = t + bit * (1 - 2 * lax.rem(lax.div(i, bit), 2))
        bit *= 2
    return t


def _kernel(X, Y, h_ref, g_ref, lens_ref, inv_ref, wq, wk, wv, w_in, wo, w_out, kc, vc,
            h_out, k_out, v_out,
            wqkv_b, win_b, wo_b, wout_b, k_b, v_b, kt_b,
            hx, hbuf0, hbuf, lens_b, inv_b, mown, mrow, xs, cos_b, sin_b, lenb,
            pq, pk, pv, rq, rv, rks, kx, rkx, q_b, m_b, d_b, of32, obuf,
            fsib, fsibr, fown, fcross, fcrossr, fbuf, yacc, ybuf, ry,
            isem, wsem, sent, hrecv, mrecv, qrecv, arecv, brecv, crecv, orecv, ysend, yrecv):
    me_y = lax.axis_index("yz")
    me_x = lax.axis_index("x")
    L = wqkv_b.shape[0]
    B, BLK = h_ref.shape
    S, D = kc.shape[2], kc.shape[3]
    HD = wq.shape[2]
    FL = w_in.shape[2]
    FH = FL // 2
    HW = FH // 2
    CW = FH // 4
    half = D // 2
    core = lax.rem(me_x, 2)
    py = [_partner(me_y, m) for m in range(Y)]
    px = [_partner(me_x, m) for m in range(X)]
    sib, mate = px[1], px[3]
    part_of_f = lax.rem(core + lax.div(me_x, 2), 2)
    masks = list(range(Y - 1, 0, -1))
    near = lax.div(me_y, Y // 2)
    total = [0]

    barrier = pltpu.get_barrier_semaphore()
    for m in masks:
        pl.semaphore_signal(barrier, inc=1, device_id=(py[m], me_x), device_id_type=MESH)
    for n in range(X - 1, 0, -1):
        pl.semaphore_signal(barrier, inc=1, device_id=(me_y, px[n]), device_id_type=MESH)

    def remote(src, dst, recv, y, x, send=None):
        if send is None:
            total[0] += math.prod(src.shape) * np.dtype(src.dtype).itemsize
        pltpu.make_async_remote_copy(src, dst, sent if send is None else send, recv,
                                     device_id=(y, x), device_id_type=MESH).start()

    def wait_bytes(ref, sem, name="wait"):
        with jax.named_scope(name):
            pltpu.make_async_copy(ref, ref, sem).wait()

    inputs = [pltpu.make_async_copy(s, d, isem) for s, d in (
        (h_ref, hx.at[pl.ds(0, B)]), (g_ref, hx.at[pl.ds(B, L)]), (lens_ref, lens_b), (inv_ref, inv_b))]
    for c in inputs:
        c.start()

    def load(w, b, l, i, parts=4):
        n = w.shape[1] // parts
        for j in range(parts):
            pltpu.make_async_copy(w.at[l, pl.ds(j * n, n)], b.at[l, pl.ds(j * n, n)], wsem.at[i]).start()

    def load_qkv(l, i):
        for j, w in enumerate((wq, wk, wv)):
            pltpu.make_async_copy(w.at[l], wqkv_b.at[l, :, pl.ds(j * HD, HD)], wsem.at[i]).start()

    def transpose_k(l):
        wait_bytes(k_b.at[l], wsem.at[3 * l], "w_k")

        def step(i, carry):
            for j in range(8):
                kt_b[i * 8 + j] = k_b[l, i * 8 + j].T
            return carry

        with jax.named_scope("kt"):
            lax.fori_loop(0, B // 8, step, 0)

    for c in inputs:
        c.wait()
    load(kc, k_b, 0, 0)
    load_qkv(0, 1)
    load(w_in, win_b, 0, 1)
    load(vc, v_b, 0, 2)
    load(w_out, wout_b, 0, 2)
    load(wo, wo_b, 0, 2, 1)
    for l in range(1, L):
        load(kc, k_b, l, 3)
        load_qkv(l, 4)
        load(w_in, win_b, l, 4)
        load(vc, v_b, l, 4)
        load(w_out, wout_b, l, 4)
        load(wo, wo_b, l, 4, 1)

    row = lax.broadcasted_iota(jnp.int32, (B, D), 0)
    lane = lax.broadcasted_iota(jnp.int32, (B, D), 1)

    def column(r):
        return jnp.sum(jnp.where(row == lane, jnp.broadcast_to(r, (B, D)), 0.0), axis=1, keepdims=True)

    def as_row(c):
        return jnp.sum(jnp.where(row == lane, jnp.broadcast_to(c, (B, D)), 0.0), axis=0, keepdims=True)

    lens_row = jnp.concatenate([lens_b[...].astype(F32), jnp.zeros((1, D - B), F32)], axis=1)
    lens_col = column(lens_row)
    lenb[...] = jnp.broadcast_to(lens_col, (B, D))
    ang = lens_col * inv_b[...]
    cos_b[...] = jnp.cos(ang)
    sn = jnp.sin(ang)
    sin_b[...] = jnp.where(lane < half, -sn, sn)

    def rope(t):
        tf = t.astype(F32)
        return (tf * cos_b[...] + pltpu.roll(tf, half, 1) * sin_b[...]).astype(BF16)

    def exchange_h(src, dst):
        for m in masks:
            remote(src, dst.at[me_y], hrecv, py[m], me_x)

    def rms(ss, n):
        return jnp.minimum(jnp.sqrt(ss / n + EPS), 1e38)

    lane1 = lax.broadcasted_iota(jnp.int32, (1, D), 1)
    NX = Y * BLK

    hbuf0[me_y] = hx[...]

    with jax.named_scope("w_bar"):
        pl.semaphore_wait(barrier, X + Y - 2)
    exchange_h(hx, hbuf0)
    transpose_k(0)

    for l in range(L):
        last = l == L - 1
        hall = hbuf if l else hbuf0
        wait_bytes(hall.at[pl.ds(0, Y - 1)], hrecv, "w_h")
        row_ss = jnp.zeros((B, BLK), F32)
        gmax = jnp.zeros((1, BLK), F32)
        for j in range(Y):
            hf = hall[j, 0:B].astype(F32)
            row_ss = row_ss + hf * hf
            gmax = jnp.maximum(gmax, jnp.abs(hbuf0[j, B + l:B + l + 1].astype(F32)))
        ss = jnp.sum(row_ss, axis=1, keepdims=True)
        G = jnp.maximum(jnp.max(gmax, axis=1, keepdims=True), 2.0 ** -100)
        mown[l] = jnp.where(lane1 == B, G, as_row(ss))
        for m in (1, 2, 3):
            remote(mown.at[l], mrow.at[l, m - 1], mrecv.at[0 if m == 1 else 1], me_y, px[m])
        sx = lax.rsqrt(ss / NX + EPS)
        for j in range(Y):
            gl = (hbuf0[j, B + l:B + l + 1].astype(F32) / G) * DOWN
            xs[:, j * BLK:(j + 1) * BLK] = (hall[j, 0:B].astype(F32) * sx * gl).astype(BF16)

        if l == 0:
            wait_bytes(wqkv_b.at[l], wsem.at[1], "w_wqkv")
            wait_bytes(win_b.at[l], wsem.at[1], "w_win")
        else:
            for b in (wqkv_b, win_b, v_b, wout_b, wo_b):
                wait_bytes(b.at[l], wsem.at[4], "w_w1")

        def part(i, dst):
            p = jnp.dot(xs[...], wqkv_b[l, :, i * HD:(i + 1) * HD], preferred_element_type=F32).astype(BF16)
            for j in range(X):
                dst[l, j] = p[:, j * D:(j + 1) * D]

        part(0, pq)
        for m in (2, 3, 1):
            remote(pq.at[l, px[m]], rq.at[l, m - 1], qrecv.at[0], me_y, px[m])
        part(1, pk)
        for i, t in enumerate((px[2], sib)):
            remote(pk.at[l, t], rks.at[l, i], qrecv.at[1], me_y, sib)
        part(2, pv)
        for m in (2, 3, 1):
            remote(pv.at[l, px[m]], rv.at[l, m - 1], qrecv.at[2], me_y, px[m])


        def f_part(c, i):
            cols = pl.ds(pl.multiple_of(c * FH + i * HW, HW), HW)
            return jnp.dot(xs[...], win_b[l, :, cols], preferred_element_type=F32)

        def f_sib(i):
            fsib[l, i] = f_part(1 - part_of_f, i).astype(BF16)
            remote(fsib.at[l, i], fsibr.at[l, i], arecv.at[i], me_y, sib)

        def f_add(i):
            wait_bytes(fsibr.at[l, i], arecv.at[i], "w_fs")
            s = fown[i] * w_own + fsibr[l, i].astype(F32) * w_sib
            fown[i] = s
            for j in range(2):
                fcross[l, 2 * i + j] = s[:, j * CW:(j + 1) * CW].astype(BF16)
            for c, (q0, nq) in enumerate(QUARTERS):
                if q0 // 2 == i:
                    qs = pl.ds(q0, nq)
                    remote(fcross.at[l, qs], fcrossr.at[l, qs], brecv.at[l, c], me_y, mate)

        f_sib(0)
        fown[0] = f_part(part_of_f, 0)
        wait_bytes(mrow.at[l, 0], mrecv.at[0], "w_ms")
        ss1, G1 = column(mrow[l, 0]), mrow[l, 0, :, B:B + 1]
        ssc, Gc = ss + ss1, jnp.maximum(G, G1)
        sc_ = lax.rsqrt(ssc / (2 * NX) + EPS)
        w_own = sc_ * rms(ss, NX) * (G / Gc)
        w_sib = sc_ * rms(ss1, NX) * (G1 / Gc)
        wait_bytes(rks.at[l], qrecv.at[1], "w_ks")
        kx[l] = (pk[l, mate].astype(F32) * w_own + rks[l, 0].astype(F32) * w_sib).astype(BF16)
        remote(kx.at[l], rkx.at[l], qrecv.at[3], me_y, mate)
        f_sib(1)
        f_add(0)
        fown[1] = f_part(part_of_f, 1)
        f_add(1)

        scale = D ** -0.5
        if l == 0:
            for b in (v_b, wout_b, wo_b):
                wait_bytes(b.at[l], wsem.at[2], "w_v")
        wait_bytes(mrow.at[l, pl.ds(1, 2)], mrecv.at[1], "w_m")
        ss2, G2 = column(mrow[l, 1]), mrow[l, 1, :, B:B + 1]
        ss3, G3 = column(mrow[l, 2]), mrow[l, 2, :, B:B + 1]
        ssd, Gd = ss2 + ss3, jnp.maximum(G2, G3)
        r = lax.rsqrt((ssc + ssd) / (4 * NX) + EPS)
        rows4 = [(r * rms(a, NX), b) for a, b in ((ss, G), (ss1, G1), (ss2, G2), (ss3, G3))]
        fc, fd = r * rms(ssc, 2 * NX), r * rms(ssd, 2 * NX)

        def joined(p, got):
            s = (p.astype(F32) * rows4[0][0]) * rows4[0][1]
            for d in range(X - 1):
                s = s + (got[d].astype(F32) * rows4[d + 1][0]) * rows4[d + 1][1]
            return (s * UP).astype(BF16)

        def chips(mine, theirs):
            return (((mine * fc) * Gc + (theirs * fd) * Gd) * UP).astype(BF16)

        wait_bytes(rq.at[l], qrecv.at[0], "w_q")
        q = rope(joined(pq[l, me_x], rq[l]))
        q_b[...] = q
        GB = 16
        grow = lax.broadcasted_iota(jnp.int32, (GB, S), 0)
        orow = lax.broadcasted_iota(jnp.int32, (GB, D), 0)
        pos = lax.broadcasted_iota(jnp.int32, (GB, S), 1).astype(F32)

        def scores(i):
            b0 = i * GB
            qg = q_b[b0:b0 + GB, :]
            acc = jnp.zeros((GB, S), F32)
            for j in range(GB):
                acc = jnp.where(grow == j, jnp.dot(qg, kt_b[b0 + j], preferred_element_type=F32), acc)
            ln = lenb[b0:b0 + GB, :]
            sc = jnp.where(pos < jnp.concatenate([ln] * (S // D), axis=1), acc * scale, -jnp.inf)
            m = jnp.max(sc, axis=1, keepdims=True)
            p = jnp.exp(sc - m)
            m_b[b0:b0 + GB, :] = jnp.broadcast_to(m, (GB, D))
            d_b[b0:b0 + GB, :] = jnp.broadcast_to(jnp.sum(p, axis=1, keepdims=True), (GB, D))
            return p.astype(BF16)

        def values(i, p):
            b0 = i * GB
            acc = jnp.zeros((GB, D), F32)
            for j in range(0, GB, 2):
                pair = jnp.concatenate([v_b[l, b0 + j], v_b[l, b0 + j + 1]], axis=1)
                t = jnp.dot(p, pair, preferred_element_type=F32)
                acc = jnp.where(orow == j, t[:, :D], jnp.where(orow == j + 1, t[:, D:], acc))
            of32[b0:b0 + GB, :] = acc

        with jax.named_scope("attn"):
            prev = scores(0)
            for i in range(1, B // GB):
                cur = scores(i)
                values(i - 1, prev)
                prev = cur

        wait_bytes(rv.at[l], qrecv.at[2], "w_nv")
        wait_bytes(rkx.at[l], qrecv.at[3], "w_nk")
        values(B // GB - 1, prev)
        v = joined(pv[l, me_x], rv[l])
        k = rope(chips(pk[l, me_x].astype(F32) * w_own + rks[l, 1].astype(F32) * w_sib, rkx[l].astype(F32)))
        sn = jnp.sum(q_b[...].astype(F32) * k.astype(F32), axis=1, keepdims=True) * scale
        m = jnp.maximum(m_b[...], sn)
        al = jnp.exp(m_b[...] - m)
        pn = jnp.exp(sn - m)
        den = d_b[...] * al + pn
        o = of32[...] * al + pn * v.astype(F32)
        obuf[l, me_x] = (o / den).astype(BF16)
        for m in (2, 3, 1):
            remote(obuf.at[l, me_x], obuf.at[l, me_x], orecv, me_y, px[m])
        k_out[l] = k
        v_out[l] = v

        def f_dot(q0, nq, cols):
            f = jnp.concatenate([fbuf[l, q0 + i] for i in range(nq)], axis=1)
            rows = pl.ds(pl.multiple_of(q0 * CW, CW), nq * CW)
            return jnp.dot(f, wout_b[l, rows, cols], preferred_element_type=F32)

        mine, other = part_of_f * 4, (1 - part_of_f) * 4
        everything = slice(None)
        for c, (q0, nq) in enumerate(QUARTERS):
            wait_bytes(fcrossr.at[l, pl.ds(q0, nq)], brecv.at[l, c], "w_fc")
            for i in range(q0, q0 + nq):
                u = chips(fown[i // 2, :, (i % 2) * CW:(i % 2 + 1) * CW], fcrossr[l, i].astype(F32))
                fbuf[l, mine + i] = _gelu(u.astype(F32)).astype(BF16)
            qs = pl.ds(mine + q0, nq)
            remote(fbuf.at[l, qs], fbuf.at[l, qs], crecv.at[c], me_y, sib)
            if c == 0:
                yacc[...] = f_dot(mine + q0, nq, everything)
            elif c == 1:
                yacc[...] = yacc[...] + f_dot(mine + q0, nq, everything)
            else:
                p0, np_ = QUARTERS[0]
                wait_bytes(fbuf.at[l, pl.ds(p0, np_)], crecv.at[0], "w_fg")
                yacc[...] = yacc[...] + (f_dot(mine + q0, nq, everything) + f_dot(other + p0, np_, everything))
        p0, np_ = QUARTERS[1]
        wait_bytes(fbuf.at[l, pl.ds(p0, np_)], crecv.at[1], "w_fg")
        yacc[...] = yacc[...] + f_dot(other + p0, np_, everything)
        wait_bytes(obuf.at[l, pl.ds(0, X - 1)], orecv, "w_og")
        og = jnp.concatenate([obuf[l, j] for j in range(X)], axis=1)
        yacc[...] = yacc[...] + jnp.dot(og, wo_b[l], preferred_element_type=F32)
        p0, np_ = QUARTERS[2]
        wait_bytes(fbuf.at[l, pl.ds(p0, np_)], crecv.at[2], "w_fg")
        W = Y // 2 * BLK
        for hz, ms in ((1 - near, masks[:Y // 2]), (near, masks[Y // 2:])):
            cols = pl.ds(pl.multiple_of(hz * W, W), W)
            acc = yacc[:, cols] + f_dot(other + p0, np_, cols)
            for j in range(Y // 2):
                ybuf[l, hz * (Y // 2) + j] = acc[:, j * BLK:(j + 1) * BLK].astype(BF16)
            for m in ms:
                remote(ybuf.at[l, py[m]], ry.at[l, m - 1], yrecv, py[m], me_x, ysend if last else None)
        if last:
            n = total[0]
            big = S * D * 2
            wait_bytes(k_b.at[0, pl.ds(0, n // big)], sent)
            if n % big:
                wait_bytes(k_b.at[0, 0, pl.ds(0, n % big // (2 * D))], sent)
            wait_bytes(ry.at[l], ysend)
        else:
            transpose_k(l + 1)
        wait_bytes(ry.at[l], yrecv, "w_y")
        y = ybuf[l, me_y].astype(F32)
        for d in range(Y - 1):
            y = y + ry[l, d].astype(F32)
        hn = (hall[me_y, 0:B].astype(F32) + y.astype(BF16).astype(F32)).astype(BF16)
        if last:
            h_out[...] = hn
        else:
            hbuf[me_y] = hn
            exchange_h(hbuf.at[me_y], hbuf)


def _finish(h, k, v, h_out, k_out, v_out, sem):
    copies = [pltpu.make_async_copy(a, b, sem.at[i]) for i, (a, b) in enumerate(((k, k_out), (v, v_out), (h, h_out)))]
    for c in copies:
        c.start()
    for c in copies:
        c.wait()


def solution(mesh):
    X = mesh.shape['x']
    Y = mesh.shape['yz']
    act = P(None, ('x', 'yz'))
    w_first = P(None, 'x', 'yz')
    w_second = P(None, 'yz', 'x')
    cache = P(None, None, ('yz', 'x'), None, None)
    new = P(None, None, ('yz', 'x'), None)

    def body(h, g, wq, wk, wv, w_in, wo, w_out, kc, vc, lens):
        B, BLK = h.shape
        L, E, HD = wq.shape
        FL = w_in.shape[2]
        S, D = kc.shape[3], kc.shape[4]
        half = D // 2
        CW = FL // 8
        kc = kc.reshape(L, B, S, D)
        vc = vc.reshape(L, B, S, D)
        i = np.arange(half, dtype=np.float32)
        inv = np.power(np.float32(10000.0), -i / np.float32(half)).astype(np.float32)
        inv = jnp.asarray(np.concatenate([inv, inv])[None])
        vm = pl.BlockSpec(memory_space=pltpu.VMEM)
        hbm = pl.BlockSpec(memory_space=pl.ANY)
        far = pl.BlockSpec(memory_space=pltpu.HBM)
        dma = pltpu.SemaphoreType.DMA
        V = pltpu.VMEM
        scratch = [
            V((L, E, 3 * HD), BF16), V((L, E, FL), BF16), V((L, HD, E), BF16), V((L, FL, E), BF16),
            V((L, B, S, D), BF16), V((L, B, S, D), BF16), V((B, D, S), BF16),
            V((B + 8, BLK), BF16), V((Y, B + 8, BLK), BF16), V((Y, B, BLK), BF16),
            V((1, B), jnp.int32), V((1, D), F32),
            V((L, 1, D), F32), V((L, X - 1, 1, D), F32), V((B, Y * BLK), BF16),
            V((B, D), F32), V((B, D), F32), V((B, D), F32),
            V((L, X, B, D), BF16), V((L, X, B, D), BF16), V((L, X, B, D), BF16),
            V((L, X - 1, B, D), BF16), V((L, X - 1, B, D), BF16), V((L, 2, B, D), BF16),
            V((L, B, D), BF16), V((L, B, D), BF16),
            V((B, D), BF16), V((B, D), F32), V((B, D), F32), V((B, D), F32), V((L, X, B, D), BF16),
            V((L, 2, B, 2 * CW), BF16), V((L, 2, B, 2 * CW), BF16), V((2, B, 2 * CW), F32),
            V((L, 4, B, CW), BF16), V((L, 4, B, CW), BF16), V((L, 8, B, CW), BF16),
            V((B, Y * BLK), F32), V((L, Y, B, BLK), BF16), V((L, Y - 1, B, BLK), BF16),
            dma, dma((5,)), dma, dma, dma((2,)), dma((4,)), dma((2,)), dma((L, NC)), dma((NC,)), dma, dma, dma,
        ]
        shapes = (jax.ShapeDtypeStruct((B, BLK), BF16),
                  jax.ShapeDtypeStruct((L, B, D), BF16),
                  jax.ShapeDtypeStruct((L, B, D), BF16))
        outs = pl.pallas_call(
            functools.partial(_kernel, X, Y),
            out_shape=tuple(V(t.shape, t.dtype) for t in shapes),
            in_specs=[hbm] * 12,
            out_specs=(vm, vm, vm),
            scratch_shapes=scratch,
            compiler_params=pltpu.CompilerParams(
                collective_id=0, has_side_effects=True, vmem_limit_bytes=56 * 1024 * 1024),
            name="decode_step",
        )(h, g, lens.reshape(1, B), inv, wq, wk, wv, w_in, wo, w_out, kc, vc)
        h_new, k_new, v_new = pl.pallas_call(
            _finish, out_shape=shapes, in_specs=[vm] * 3, out_specs=(far, far, far), name="finish",
            scratch_shapes=[dma((3,))],
        )(*[pltpu.with_memory_space_constraint(t, pltpu.VMEM) for t in outs])
        return h_new, k_new.reshape(L, B, 1, D), v_new.reshape(L, B, 1, D)

    return jax.shard_map(
        body, mesh=mesh,
        in_specs=(act, act, w_first, w_first, w_first, w_first, w_second, w_second, cache, cache, P(None)),
        out_specs=(act, new, new), check_vma=False)
```

```python
import functools
import math

import numpy as np

import jax
import jax.numpy as jnp
from jax import lax
from jax.experimental import pallas as pl
from jax.experimental.pallas import tpu as pltpu
from jax.sharding import PartitionSpec as P

EPS = 1e-6
MESH = pl.DeviceIdType.MESH
F32 = jnp.float32
BF16 = jnp.bfloat16
QUARTERS = ((0, 2), (2, 1), (3, 1))
NC = len(QUARTERS)
UP, DOWN = 2.0 ** 18, 2.0 ** -18


def _gelu(x):
    return 0.5 * x * (1.0 + jnp.tanh(math.sqrt(2.0 / math.pi) * (x + 0.044715 * (x * x * x))))


def _partner(i, mask):
    bit = 1
    t = i
    while bit <= mask:
        if mask & bit:
            t = t + bit * (1 - 2 * lax.rem(lax.div(i, bit), 2))
        bit *= 2
    return t


def _kernel(X, Y, h_ref, g_ref, lens_ref, inv_ref, wq, wk, wv, w_in, wo, w_out, kc, vc,
            h_out, k_out, v_out,
            wqkv_b, win_b, wo_b, wout_b, k_b, v_b, kt_b,
            hx, hbuf0, hbuf, lens_b, inv_b, mown, mrow, xs, cos_b, sin_b, lenb,
            pq, pk, pv, rq, rv, rks, kx, rkx, q_b, m_b, d_b, of32, obuf,
            fsib, fsibr, fown, fcross, fcrossr, fbuf, yacc, ybuf, ry,
            wsem, sent, hrecv, mrecv, qrecv, arecv, brecv, crecv, orecv, yrecv):
    me_y = lax.axis_index("yz")
    me_x = lax.axis_index("x")
    L = wqkv_b.shape[0]
    B, BLK = h_ref.shape
    S, D = kc.shape[2], kc.shape[3]
    HD = wq.shape[2]
    FL = w_in.shape[2]
    FH = FL // 2
    HW = FH // 2
    CW = FH // 4
    half = D // 2
    core = lax.rem(me_x, 2)
    py = [_partner(me_y, m) for m in range(Y)]
    px = [_partner(me_x, m) for m in range(X)]
    sib, mate = px[1], px[3]
    part_of_f = lax.rem(core + lax.div(me_x, 2), 2)
    masks = list(range(Y - 1, 0, -1))
    total = [0]

    barrier = pltpu.get_barrier_semaphore()
    for m in masks:
        pl.semaphore_signal(barrier, inc=1, device_id=(py[m], me_x), device_id_type=MESH)
    for n in range(X - 1, 0, -1):
        pl.semaphore_signal(barrier, inc=1, device_id=(me_y, px[n]), device_id_type=MESH)

    def remote(src, dst, recv, y, x):
        total[0] += math.prod(src.shape) * np.dtype(src.dtype).itemsize
        pltpu.make_async_remote_copy(src, dst, sent, recv, device_id=(y, x), device_id_type=MESH).start()

    def wait_bytes(ref, sem, name="wait"):
        with jax.named_scope(name):
            pltpu.make_async_copy(ref, ref, sem).wait()

    inputs = [pltpu.make_async_copy(s, d, wsem.at[0]) for s, d in (
        (h_ref, hx.at[pl.ds(0, B)]), (g_ref, hx.at[pl.ds(B, L)]), (lens_ref, lens_b), (inv_ref, inv_b))]
    for c in inputs:
        c.start()

    def load(w, b, l, i, parts=4):
        n = w.shape[1] // parts
        for j in range(parts):
            pltpu.make_async_copy(w.at[l, pl.ds(j * n, n)], b.at[l, pl.ds(j * n, n)], wsem.at[i]).start()

    def load_qkv(l, i):
        for j, w in enumerate((wq, wk, wv)):
            pltpu.make_async_copy(w.at[l], wqkv_b.at[l, :, pl.ds(j * HD, HD)], wsem.at[i]).start()

    def transpose_k(l):
        wait_bytes(k_b.at[l], wsem.at[3 * l], "w_k")

        def step(i, carry):
            for j in range(8):
                kt_b[i * 8 + j] = k_b[l, i * 8 + j].T
            return carry

        with jax.named_scope("kt"):
            lax.fori_loop(0, B // 8, step, 0)

    for c in inputs:
        c.wait()
    load(kc, k_b, 0, 0)
    load_qkv(0, 1)
    load(w_in, win_b, 0, 1)
    load(vc, v_b, 0, 2)
    load(w_out, wout_b, 0, 2)
    load(wo, wo_b, 0, 2, 1)
    for l in range(1, L):
        load(kc, k_b, l, 3)
        load_qkv(l, 4)
        load(w_in, win_b, l, 4)
        load(vc, v_b, l, 4)
        load(w_out, wout_b, l, 4)
        load(wo, wo_b, l, 4, 1)

    row = lax.broadcasted_iota(jnp.int32, (B, D), 0)
    lane = lax.broadcasted_iota(jnp.int32, (B, D), 1)

    def column(r):
        return jnp.sum(jnp.where(row == lane, jnp.broadcast_to(r, (B, D)), 0.0), axis=1, keepdims=True)

    def as_row(c):
        return jnp.sum(jnp.where(row == lane, jnp.broadcast_to(c, (B, D)), 0.0), axis=0, keepdims=True)

    lens_row = jnp.concatenate([lens_b[...].astype(F32), jnp.zeros((1, D - B), F32)], axis=1)
    lens_col = column(lens_row)
    lenb[...] = jnp.broadcast_to(lens_col, (B, D))
    ang = lens_col * inv_b[...]
    cos_b[...] = jnp.cos(ang)
    sn = jnp.sin(ang)
    sin_b[...] = jnp.where(lane < half, -sn, sn)

    def rope(t):
        tf = t.astype(F32)
        return (tf * cos_b[...] + pltpu.roll(tf, half, 1) * sin_b[...]).astype(BF16)

    def exchange_h(src, dst):
        for m in masks:
            remote(src, dst.at[me_y], hrecv, py[m], me_x)

    def rms(ss, n):
        return jnp.minimum(jnp.sqrt(ss / n + EPS), 1e38)

    lane1 = lax.broadcasted_iota(jnp.int32, (1, D), 1)
    NX = Y * BLK

    hbuf0[me_y] = hx[...]

    with jax.named_scope("w_bar"):
        pl.semaphore_wait(barrier, X + Y - 2)
    exchange_h(hx, hbuf0)
    transpose_k(0)

    for l in range(L):
        last = l == L - 1
        hall = hbuf if l else hbuf0
        wait_bytes(hall.at[pl.ds(0, Y - 1)], hrecv, "w_h")
        row_ss = jnp.zeros((B, BLK), F32)
        gmax = jnp.zeros((1, BLK), F32)
        for j in range(Y):
            hf = hall[j, 0:B].astype(F32)
            row_ss = row_ss + hf * hf
            gmax = jnp.maximum(gmax, jnp.abs(hbuf0[j, B + l:B + l + 1].astype(F32)))
        ss = jnp.sum(row_ss, axis=1, keepdims=True)
        G = jnp.maximum(jnp.max(gmax, axis=1, keepdims=True), 2.0 ** -100)
        mown[l] = jnp.where(lane1 == B, G, as_row(ss))
        for m in (1, 2, 3):
            remote(mown.at[l], mrow.at[l, m - 1], mrecv.at[0 if m == 1 else 1], me_y, px[m])
        sx = lax.rsqrt(ss / NX + EPS)
        for j in range(Y):
            gl = (hbuf0[j, B + l:B + l + 1].astype(F32) / G) * DOWN
            xs[:, j * BLK:(j + 1) * BLK] = (hall[j, 0:B].astype(F32) * sx * gl).astype(BF16)

        if l == 0:
            wait_bytes(wqkv_b.at[l], wsem.at[1], "w_wqkv")
            wait_bytes(win_b.at[l], wsem.at[1], "w_win")
        else:
            for b in (wqkv_b, win_b, v_b, wout_b, wo_b):
                wait_bytes(b.at[l], wsem.at[4], "w_w1")

        def part(i, dst):
            p = jnp.dot(xs[...], wqkv_b[l, :, i * HD:(i + 1) * HD], preferred_element_type=F32).astype(BF16)
            for j in range(X):
                dst[l, j] = p[:, j * D:(j + 1) * D]

        part(0, pq)
        for m in (2, 3, 1):
            remote(pq.at[l, px[m]], rq.at[l, m - 1], qrecv.at[0], me_y, px[m])
        part(1, pk)
        for i, t in enumerate((px[2], sib)):
            remote(pk.at[l, t], rks.at[l, i], qrecv.at[1], me_y, sib)
        part(2, pv)
        for m in (2, 3, 1):
            remote(pv.at[l, px[m]], rv.at[l, m - 1], qrecv.at[2], me_y, px[m])


        def f_part(c, i):
            cols = pl.ds(pl.multiple_of(c * FH + i * HW, HW), HW)
            return jnp.dot(xs[...], win_b[l, :, cols], preferred_element_type=F32)

        def f_sib(i):
            fsib[l, i] = f_part(1 - part_of_f, i).astype(BF16)
            remote(fsib.at[l, i], fsibr.at[l, i], arecv.at[i], me_y, sib)

        def f_add(i):
            wait_bytes(fsibr.at[l, i], arecv.at[i], "w_fs")
            s = fown[i] * w_own + fsibr[l, i].astype(F32) * w_sib
            fown[i] = s
            for j in range(2):
                fcross[l, 2 * i + j] = s[:, j * CW:(j + 1) * CW].astype(BF16)
            for c, (q0, nq) in enumerate(QUARTERS):
                if q0 // 2 == i:
                    qs = pl.ds(q0, nq)
                    remote(fcross.at[l, qs], fcrossr.at[l, qs], brecv.at[l, c], me_y, mate)

        f_sib(0)
        fown[0] = f_part(part_of_f, 0)
        wait_bytes(mrow.at[l, 0], mrecv.at[0], "w_ms")
        ss1, G1 = column(mrow[l, 0]), mrow[l, 0, :, B:B + 1]
        ssc, Gc = ss + ss1, jnp.maximum(G, G1)
        sc_ = lax.rsqrt(ssc / (2 * NX) + EPS)
        w_own = sc_ * rms(ss, NX) * (G / Gc)
        w_sib = sc_ * rms(ss1, NX) * (G1 / Gc)
        wait_bytes(rks.at[l], qrecv.at[1], "w_ks")
        kx[l] = (pk[l, mate].astype(F32) * w_own + rks[l, 0].astype(F32) * w_sib).astype(BF16)
        remote(kx.at[l], rkx.at[l], qrecv.at[3], me_y, mate)
        f_sib(1)
        f_add(0)
        fown[1] = f_part(part_of_f, 1)
        f_add(1)

        scale = D ** -0.5
        if l == 0:
            for b in (v_b, wout_b, wo_b):
                wait_bytes(b.at[l], wsem.at[2], "w_v")
        wait_bytes(mrow.at[l, pl.ds(1, 2)], mrecv.at[1], "w_m")
        ss2, G2 = column(mrow[l, 1]), mrow[l, 1, :, B:B + 1]
        ss3, G3 = column(mrow[l, 2]), mrow[l, 2, :, B:B + 1]
        ssd, Gd = ss2 + ss3, jnp.maximum(G2, G3)
        r = lax.rsqrt((ssc + ssd) / (4 * NX) + EPS)
        rows4 = [(r * rms(a, NX), b) for a, b in ((ss, G), (ss1, G1), (ss2, G2), (ss3, G3))]
        fc, fd = r * rms(ssc, 2 * NX), r * rms(ssd, 2 * NX)

        def joined(p, got):
            s = (p.astype(F32) * rows4[0][0]) * rows4[0][1]
            for d in range(X - 1):
                s = s + (got[d].astype(F32) * rows4[d + 1][0]) * rows4[d + 1][1]
            return (s * UP).astype(BF16)

        def chips(mine, theirs):
            return (((mine * fc) * Gc + (theirs * fd) * Gd) * UP).astype(BF16)

        wait_bytes(rq.at[l], qrecv.at[0], "w_q")
        q = rope(joined(pq[l, me_x], rq[l]))
        q_b[...] = q
        GB = 16
        grow = lax.broadcasted_iota(jnp.int32, (GB, S), 0)
        orow = lax.broadcasted_iota(jnp.int32, (GB, D), 0)
        pos = lax.broadcasted_iota(jnp.int32, (GB, S), 1).astype(F32)

        def scores(i):
            b0 = i * GB
            qg = q_b[b0:b0 + GB, :]
            acc = jnp.zeros((GB, S), F32)
            for j in range(GB):
                acc = jnp.where(grow == j, jnp.dot(qg, kt_b[b0 + j], preferred_element_type=F32), acc)
            ln = lenb[b0:b0 + GB, :]
            sc = jnp.where(pos < jnp.concatenate([ln] * (S // D), axis=1), acc * scale, -jnp.inf)
            m = jnp.max(sc, axis=1, keepdims=True)
            p = jnp.exp(sc - m)
            m_b[b0:b0 + GB, :] = jnp.broadcast_to(m, (GB, D))
            d_b[b0:b0 + GB, :] = jnp.broadcast_to(jnp.sum(p, axis=1, keepdims=True), (GB, D))
            return p.astype(BF16)

        def values(i, p):
            b0 = i * GB
            acc = jnp.zeros((GB, D), F32)
            for j in range(0, GB, 2):
                pair = jnp.concatenate([v_b[l, b0 + j], v_b[l, b0 + j + 1]], axis=1)
                t = jnp.dot(p, pair, preferred_element_type=F32)
                acc = jnp.where(orow == j, t[:, :D], jnp.where(orow == j + 1, t[:, D:], acc))
            of32[b0:b0 + GB, :] = acc

        with jax.named_scope("attn"):
            prev = scores(0)
            for i in range(1, B // GB):
                cur = scores(i)
                values(i - 1, prev)
                prev = cur

        wait_bytes(rv.at[l], qrecv.at[2], "w_nv")
        wait_bytes(rkx.at[l], qrecv.at[3], "w_nk")
        values(B // GB - 1, prev)
        v = joined(pv[l, me_x], rv[l])
        k = rope(chips(pk[l, me_x].astype(F32) * w_own + rks[l, 1].astype(F32) * w_sib, rkx[l].astype(F32)))
        sn = jnp.sum(q_b[...].astype(F32) * k.astype(F32), axis=1, keepdims=True) * scale
        m = jnp.maximum(m_b[...], sn)
        al = jnp.exp(m_b[...] - m)
        pn = jnp.exp(sn - m)
        den = d_b[...] * al + pn
        o = of32[...] * al + pn * v.astype(F32)
        obuf[l, me_x] = (o / den).astype(BF16)
        for m in (2, 3, 1):
            remote(obuf.at[l, me_x], obuf.at[l, me_x], orecv, me_y, px[m])
        k_out[l] = k
        v_out[l] = v

        def f_dot(q0, nq, cols):
            f = jnp.concatenate([fbuf[l, q0 + i] for i in range(nq)], axis=1)
            rows = pl.ds(pl.multiple_of(q0 * CW, CW), nq * CW)
            return jnp.dot(f, wout_b[l, rows, cols], preferred_element_type=F32)

        mine, other = part_of_f * 4, (1 - part_of_f) * 4
        everything = slice(None)
        for c, (q0, nq) in enumerate(QUARTERS):
            wait_bytes(fcrossr.at[l, pl.ds(q0, nq)], brecv.at[l, c], "w_fc")
            for i in range(q0, q0 + nq):
                u = chips(fown[i // 2, :, (i % 2) * CW:(i % 2 + 1) * CW], fcrossr[l, i].astype(F32))
                fbuf[l, mine + i] = _gelu(u.astype(F32)).astype(BF16)
            qs = pl.ds(mine + q0, nq)
            remote(fbuf.at[l, qs], fbuf.at[l, qs], crecv.at[c], me_y, sib)
            if c == 0:
                yacc[...] = f_dot(mine + q0, nq, everything)
            elif c == 1:
                yacc[...] = yacc[...] + f_dot(mine + q0, nq, everything)
            else:
                p0, np_ = QUARTERS[0]
                wait_bytes(fbuf.at[l, pl.ds(p0, np_)], crecv.at[0], "w_fg")
                yacc[...] = yacc[...] + (f_dot(mine + q0, nq, everything) + f_dot(other + p0, np_, everything))
        p0, np_ = QUARTERS[1]
        wait_bytes(fbuf.at[l, pl.ds(p0, np_)], crecv.at[1], "w_fg")
        yacc[...] = yacc[...] + f_dot(other + p0, np_, everything)
        wait_bytes(obuf.at[l, pl.ds(0, X - 1)], orecv, "w_og")
        og = jnp.concatenate([obuf[l, j] for j in range(X)], axis=1)
        yacc[...] = yacc[...] + jnp.dot(og, wo_b[l], preferred_element_type=F32)
        p0, np_ = QUARTERS[2]
        wait_bytes(fbuf.at[l, pl.ds(p0, np_)], crecv.at[2], "w_fg")
        W = 2 * BLK
        for c in range(Y // 2):
            z = lax.div(py[masks[2 * c]], 2)
            cols = pl.ds(pl.multiple_of(z * W, W), W)
            acc = yacc[:, cols] + f_dot(other + p0, np_, cols)
            for j in range(2):
                ybuf[l, z * 2 + j] = acc[:, j * BLK:(j + 1) * BLK].astype(BF16)
            for m in masks[2 * c:2 * c + 2]:
                remote(ybuf.at[l, py[m]], ry.at[l, m - 1], yrecv, py[m], me_x)
        if last:
            n = total[0]
            big = S * D * 2
            wait_bytes(k_b.at[0, pl.ds(0, n // big)], sent)
            if n % big:
                wait_bytes(k_b.at[0, 0, pl.ds(0, n % big // (2 * D))], sent)
        else:
            transpose_k(l + 1)
        wait_bytes(ry.at[l], yrecv, "w_y")
        y = ybuf[l, me_y].astype(F32)
        for d in range(Y - 1):
            y = y + ry[l, d].astype(F32)
        hn = (hall[me_y, 0:B].astype(F32) + y.astype(BF16).astype(F32)).astype(BF16)
        if last:
            h_out[...] = hn
        else:
            hbuf[me_y] = hn
            exchange_h(hbuf.at[me_y], hbuf)


def _finish(h, k, v, h_out, k_out, v_out, sem):
    copies = [pltpu.make_async_copy(a, b, sem.at[i]) for i, (a, b) in enumerate(((k, k_out), (v, v_out), (h, h_out)))]
    for c in copies:
        c.start()
    for c in copies:
        c.wait()


def solution(mesh):
    X = mesh.shape['x']
    Y = mesh.shape['yz']
    act = P(None, ('x', 'yz'))
    w_first = P(None, 'x', 'yz')
    w_second = P(None, 'yz', 'x')
    cache = P(None, None, ('yz', 'x'), None, None)
    new = P(None, None, ('yz', 'x'), None)

    def body(h, g, wq, wk, wv, w_in, wo, w_out, kc, vc, lens):
        B, BLK = h.shape
        L, E, HD = wq.shape
        FL = w_in.shape[2]
        S, D = kc.shape[3], kc.shape[4]
        half = D // 2
        CW = FL // 8
        kc = kc.reshape(L, B, S, D)
        vc = vc.reshape(L, B, S, D)
        i = np.arange(half, dtype=np.float32)
        inv = np.power(np.float32(10000.0), -i / np.float32(half)).astype(np.float32)
        inv = jnp.asarray(np.concatenate([inv, inv])[None])
        vm = pl.BlockSpec(memory_space=pltpu.VMEM)
        hbm = pl.BlockSpec(memory_space=pl.ANY)
        far = pl.BlockSpec(memory_space=pltpu.HBM)
        dma = pltpu.SemaphoreType.DMA
        V = pltpu.VMEM
        scratch = [
            V((L, E, 3 * HD), BF16), V((L, E, FL), BF16), V((L, HD, E), BF16), V((L, FL, E), BF16),
            V((L, B, S, D), BF16), V((L, B, S, D), BF16), V((B, D, S), BF16),
            V((B + 8, BLK), BF16), V((Y, B + 8, BLK), BF16), V((Y, B, BLK), BF16),
            V((1, B), jnp.int32), V((1, D), F32),
            V((L, 1, D), F32), V((L, X - 1, 1, D), F32), V((B, Y * BLK), BF16),
            V((B, D), F32), V((B, D), F32), V((B, D), F32),
            V((L, X, B, D), BF16), V((L, X, B, D), BF16), V((L, X, B, D), BF16),
            V((L, X - 1, B, D), BF16), V((L, X - 1, B, D), BF16), V((L, 2, B, D), BF16),
            V((L, B, D), BF16), V((L, B, D), BF16),
            V((B, D), BF16), V((B, D), F32), V((B, D), F32), V((B, D), F32), V((L, X, B, D), BF16),
            V((L, 2, B, 2 * CW), BF16), V((L, 2, B, 2 * CW), BF16), V((2, B, 2 * CW), F32),
            V((L, 4, B, CW), BF16), V((L, 4, B, CW), BF16), V((L, 8, B, CW), BF16),
            V((B, Y * BLK), F32), V((L, Y, B, BLK), BF16), V((L, Y - 1, B, BLK), BF16),
            dma((5,)), dma, dma, dma((2,)), dma((4,)), dma((2,)), dma((L, NC)), dma((NC,)), dma, dma,
        ]
        shapes = (jax.ShapeDtypeStruct((B, BLK), BF16),
                  jax.ShapeDtypeStruct((L, B, D), BF16),
                  jax.ShapeDtypeStruct((L, B, D), BF16))
        outs = pl.pallas_call(
            functools.partial(_kernel, X, Y),
            out_shape=tuple(V(t.shape, t.dtype) for t in shapes),
            in_specs=[hbm] * 12,
            out_specs=(vm, vm, vm),
            scratch_shapes=scratch,
            compiler_params=pltpu.CompilerParams(
                collective_id=0, has_side_effects=True, vmem_limit_bytes=56 * 1024 * 1024),
            name="decode_step",
        )(h, g, lens.reshape(1, B), inv, wq, wk, wv, w_in, wo, w_out, kc, vc)
        h_new, k_new, v_new = pl.pallas_call(
            _finish, out_shape=shapes, in_specs=[vm] * 3, out_specs=(far, far, far), name="finish",
            scratch_shapes=[dma((3,))],
        )(*[pltpu.with_memory_space_constraint(t, pltpu.VMEM) for t in outs])
        return h_new, k_new.reshape(L, B, 1, D), v_new.reshape(L, B, 1, D)

    return jax.shard_map(
        body, mesh=mesh,
        in_specs=(act, act, w_first, w_first, w_first, w_first, w_second, w_second, cache, cache, P(None)),
        out_specs=(act, new, new), check_vma=False)
```
